512 devices in a mesh: gy: 64 (over z, y_lo, core), gz: 8 (over y_hi, x).
Axes of the slice: x: 4, y: 8 (y_hi: 2, y_lo: 4; y = y_hi * 4 + y_lo), z: 8, core: 2. Of those that a mesh axis runs over, the one named last changes fastest.
Arguments:
- omega: float32 [3, 1024, 512, 128], P(None, 'gy', 'gz'), may hold values from -6 to 6
- velocity: float32 [3, 1024, 512, 128], P(None, 'gy', 'gz'), may hold values from -6 to 6
- point_owner: int32 [1152], replicated, may hold values from 2 to 477, as said below
- point_cells: int32 [3, 1152], replicated, may hold values from 1 to 125, as said below
- point_frac: float32 [3, 1152], replicated, may hold values from 0 to 1
- chord: float32 [1152], replicated, may hold values from 0.2 to 1
- twist: float32 [1152], replicated, may hold values from -0.3 to 0.3
- angle_step: int32 [1], replicated, may hold values from 0 to 719
Outputs:
- omega_out: float32 [3, 1024, 512, 128], P(None, 'gy', 'gz')
- blade_sources: float32 [3, 1152], replicated
The draws below stay inside these ranges and needn't reach their ends.
Inputs may be any that keep to these rules, and one draw needn't show every extreme that they name: `point_owner`: turbine t's points lie in spanwise blocks t * 10 to (t + 1) * 10 - 1 and in the 4 vertical blocks from (4) // 2 on; no block holds more than 9 points, and in every turbine one block holds exactly 9. `point_cells`: streamwise cells lie in 1 to 125, spanwise in 1 to 13, vertical in 1 to 61; all points of a turbine share one streamwise cell.
All inputs are finite; a program needn't handle non-finite values.
Results may differ from the reference program's by a relative error of at most 0.0003.
Values sent between devices are 32-bit elements; how exact they have to be, the bound alone decides.
A program may use at most 128 MiB of HBM per device.

```python
import math
import jax
import jax.numpy as jnp
from jax import lax

CY = 16
CZ = 64
NX = 128
TURBINES = 6
BLADES = 3
BP = 64
NY = 1024
NZ = 512
POINTS = 1152
MOST = 9
N_GZ = 8


def rotor_layout(key):
    span_count = NY // CY
    vert_count = NZ // CZ
    span_blocks = span_count // TURBINES
    vert_blocks = max(vert_count // 2, 1)
    blocks = span_blocks * vert_blocks
    slots = blocks * MOST
    per_rotor = BLADES * BP

    def one_rotor(rotor_key, rotor_number):
        chosen = jax.random.randint(jax.random.fold_in(rotor_key, 1), (), 0, blocks)
        packed = jnp.where(rotor_number == 0, 0, jnp.where(rotor_number == TURBINES - 1, blocks - 1, chosen))
        shuffle = jax.random.permutation(jax.random.fold_in(rotor_key, 2), slots).astype(jnp.int32)
        slot_block = jnp.arange(slots, dtype=jnp.int32) // MOST
        ranking = shuffle - slots * (slot_block == packed).astype(jnp.int32)
        order = jnp.argsort(ranking, stable=True)[:per_rotor]
        return (order // MOST).astype(jnp.int32)
    rotor_keys = jax.random.split(jax.random.fold_in(key, 77), TURBINES)
    rotor_numbers = jnp.arange(TURBINES, dtype=jnp.int32)
    block = jax.vmap(one_rotor)(rotor_keys, rotor_numbers)
    rotor = rotor_numbers[:, None]
    span_index = rotor * span_blocks + block // vert_blocks
    vert_index = (vert_count - vert_blocks) // 2 + block % vert_blocks
    owner = (span_index * vert_count + vert_index).reshape(-1).astype(jnp.int32)
    cell_key = jax.random.fold_in(key, 78)
    plane = jax.random.randint(jax.random.fold_in(cell_key, 1), (TURBINES, 1), 1, NX - 2)
    cell_x = jnp.broadcast_to(plane, (TURBINES, per_rotor)).reshape(-1)
    cell_y = jax.random.randint(jax.random.fold_in(cell_key, 2), (TURBINES * per_rotor,), 1, CY - 2)
    cell_z = jax.random.randint(jax.random.fold_in(cell_key, 3), (TURBINES * per_rotor,), 1, CZ - 2)
    cells = jnp.stack([cell_x, cell_y, cell_z]).astype(jnp.int32)
    return (owner, cells)


def draw_point_owner(key, part):
    return rotor_layout(key)[0]


def draw_point_cells(key, part):
    return rotor_layout(key)[1]


def shard_levels(rng, extent, pieces, low, high):
    def one(dim, blocks):
        steps = jax.random.uniform(jax.random.fold_in(jax.random.fold_in(rng, 6), dim), (blocks,), jnp.float32, low / len(pieces), high / len(pieces))
        return jnp.repeat(jnp.exp(steps), extent[dim] // blocks).reshape((-1,) + (1,) * (len(extent) - dim - 1))

    gain = one(*pieces[0])
    for cut in pieces[1:]:
        gain = gain * one(*cut)
    return gain


def scatter_about(rng, dims, deviation, limit, pieces=(), kind=jnp.bfloat16):
    factor_of = shard_levels(rng, dims, pieces, -0.22, 0.18) if pieces else 1.0
    values = jax.random.normal(rng, dims, jnp.float32) * deviation * factor_of
    return jnp.minimum(jnp.maximum(values, -limit), limit).astype(kind)


def setup_inputs(seed: int = 0) -> dict:
    splits = jax.random.split(jax.random.key(seed), 9)
    omega = scatter_about(splits[0], (3, NY, NZ, NX), 1.0, 6.0, ((1, 64), (2, 8)), jnp.float32)
    velocity = scatter_about(splits[1], (3, NY, NZ, NX), 1.0, 6.0, ((1, 64), (2, 8)), jnp.float32)
    point_owner = draw_point_owner(jax.random.fold_in(splits[8], 71), 0)
    point_cells = draw_point_cells(jax.random.fold_in(splits[8], 71), 0)
    point_frac = jnp.clip(jax.random.uniform(splits[4], (3, POINTS), jnp.float32, 0.0, 1.0), 0.0, 1.0)
    chord = jnp.clip(jnp.exp(jax.random.uniform(splits[5], (POINTS,), jnp.float32, math.log(0.2), math.log(1.0))), 0.2, 1.0)
    twist = jnp.clip(jax.random.uniform(splits[6], (POINTS,), jnp.float32, -0.3, 0.3), -0.3, 0.3)
    angle_step = jax.random.randint(splits[7], (1,), 0, 720).astype(jnp.int32)
    return dict(omega=omega, velocity=velocity, point_owner=point_owner, point_cells=point_cells, point_frac=point_frac, chord=chord, twist=twist, angle_step=angle_step)


section_step = 0.4
viscosity = 0.05
tip_speed = 3.0
turn_step = 2.0 * 3.141592653589793 / 720.0

def remesh_kernel(shift):
    mag = jnp.abs(shift)
    inner = 1.0 - 2.5 * mag * mag + 1.5 * mag * mag * mag
    outer = 0.5 * (2.0 - mag) * (2.0 - mag) * (1.0 - mag)
    return jnp.where(mag < 1.0, inner, jnp.where(mag < 2.0, outer, 0.0))

def shifted(padded, axis, offset):
    index = []
    for dim in range(4):
        if dim == 0:
            index.append(slice(None))
        elif dim == axis:
            index.append(slice(offset, offset + padded.shape[dim] - 4))
        else:
            index.append(slice(2, padded.shape[dim] - 2))
    return padded[tuple(index)]

def centered_first(padded, axis):
    return (shifted(padded, axis, 0) - 8.0 * shifted(padded, axis, 1) + 8.0 * shifted(padded, axis, 3) - shifted(padded, axis, 4)) / 12.0

def centered_second(padded, axis):
    return (-shifted(padded, axis, 0) + 16.0 * shifted(padded, axis, 1) - 30.0 * shifted(padded, axis, 2) + 16.0 * shifted(padded, axis, 3) - shifted(padded, axis, 4)) / 12.0

def remesh_padded(field, displace, axis):
    length = field.shape[axis] - 4
    total = jnp.zeros(field.shape[:axis] + (length,) + field.shape[axis + 1:], jnp.float32)
    for offset in range(-2, 3):
        start = 2 - offset
        part = lax.slice_in_dim(field, start, start + length, axis=axis)
        moved = lax.slice_in_dim(displace, start, start + length, axis=axis - 1)
        total = total + remesh_kernel(offset - moved)[None] * part
    return total

def blade_forces(point_velocity, chord, twist, angle_step):
    count = point_velocity.shape[1]
    points = jnp.arange(count, dtype=jnp.int32)
    station = points % BP
    blade = points // BP % BLADES
    theta = angle_step[0].astype(jnp.float32) * turn_step + 2.0 * 3.141592653589793 / 3.0 * blade.astype(jnp.float32)
    radius = (station.astype(jnp.float32) + 0.5) / BP
    cos_t = jnp.cos(theta)
    sin_t = jnp.sin(theta)
    rel_x = point_velocity[0]
    rel_y = point_velocity[1] + tip_speed * radius * sin_t
    rel_z = point_velocity[2] - tip_speed * radius * cos_t
    rel_t = -sin_t * rel_y + cos_t * rel_z
    speed = jnp.sqrt(rel_x * rel_x + rel_t * rel_t + 1.0)
    gamma = 3.141592653589793 * chord * (rel_x * jnp.cos(twist) + rel_t * jnp.sin(twist))
    blades = gamma.reshape(-1, BP)
    before = jnp.concatenate([jnp.zeros((blades.shape[0], 1), jnp.float32), blades[:, :-1]], axis=1)
    shed = (blades - before).reshape(-1)
    return jnp.stack([shed * rel_x / speed, gamma * cos_t + shed * rel_y / speed, gamma * sin_t + shed * rel_z / speed])

def reference(omega, velocity, point_owner, point_cells, point_frac, chord, twist, angle_step):
    owner_span = point_owner // N_GZ
    owner_vert = point_owner % N_GZ
    base_x = point_cells[0]
    base_y = owner_span * CY + point_cells[1]
    base_z = owner_vert * CZ + point_cells[2]
    steps = jnp.arange(-1, 3, dtype=jnp.int32)
    off_x = jnp.repeat(steps, 16)
    off_y = jnp.tile(jnp.repeat(steps, 4), 4)
    off_z = jnp.tile(steps, 16)
    index_x = (base_x[None, :] + off_x[:, None]).astype(jnp.int32)
    index_y = (base_y[None, :] + off_y[:, None]).astype(jnp.int32)
    index_z = (base_z[None, :] + off_z[:, None]).astype(jnp.int32)
    weight = remesh_kernel(off_x[:, None].astype(jnp.float32) - point_frac[0][None, :])
    weight = weight * remesh_kernel(off_y[:, None].astype(jnp.float32) - point_frac[1][None, :])
    weight = weight * remesh_kernel(off_z[:, None].astype(jnp.float32) - point_frac[2][None, :])
    sampled = velocity[:, index_y, index_z, index_x]
    point_velocity = lax.optimization_barrier(jnp.sum(sampled * weight[None], axis=1))
    sources = blade_forces(point_velocity, chord, twist, angle_step)
    smear = jnp.zeros_like(omega).at[:, index_y, index_z, index_x].add(sources[:, None, :] * weight[None])
    pads = ((0, 0), (2, 2), (2, 2), (2, 2))
    omega_pad = jnp.pad(omega, pads)
    velocity_pad = jnp.pad(velocity, pads)
    stretch = jnp.zeros_like(omega)
    laplace = jnp.zeros_like(omega)
    for axis in range(3):
        stretch = stretch + omega[2 - axis][None] * centered_first(velocity_pad, 3 - axis)
        laplace = laplace + centered_second(omega_pad, axis + 1)
    section = omega + section_step * (stretch + viscosity * laplace + smear)
    displace = jnp.clip(section_step * velocity, -1.0, 1.0)
    moved_x = remesh_padded(jnp.pad(section, ((0, 0), (0, 0), (0, 0), (2, 2))), jnp.pad(displace[0], ((0, 0), (0, 0), (2, 2))), 3)
    moved_y = remesh_padded(jnp.pad(moved_x, ((0, 0), (2, 2), (0, 0), (0, 0))), jnp.pad(displace[1], ((2, 2), (0, 0), (0, 0))), 1)
    moved_z = remesh_padded(jnp.pad(moved_y, ((0, 0), (0, 0), (2, 2), (0, 0))), jnp.pad(displace[2], ((0, 0), (2, 2), (0, 0))), 2)
    return (moved_z, sources)
```

```python
import functools

import jax
import jax.numpy as jnp
from jax import lax
from jax.experimental import pallas as pl
from jax.experimental.pallas import tpu as pltpu
from jax.sharding import PartitionSpec as P

TURBINES = 6
BLADES = 3
BP = 64
MESH = pl.DeviceIdType.MESH
HI = lax.Precision.HIGHEST

section_step = 0.4
viscosity = 0.05
tip_speed = 3.0
turn_step = 2.0 * 3.141592653589793 / 720.0
F32 = jnp.float32
BF = jnp.bfloat16

CHUNK = 32


def m4(shift):
    mag = jnp.abs(shift)
    inner = 1.0 + mag * mag * (1.5 * mag - 2.5)
    far = 2.0 - mag
    outer = 0.5 * far * far * (1.0 - mag)
    return jnp.where(mag < 1.0, inner, jnp.where(mag < 2.0, outer, 0.0))


def remesh_weights(v):
    a = jnp.minimum(section_step * jnp.abs(v), 1.0)
    b = 1.0 - a
    a2 = a * a
    b2 = b * b
    w0 = 1.0 + a2 * (1.5 * a - 2.5)
    w1 = 1.0 + b2 * (1.5 * b - 2.5)
    wm = -0.5 * a * b2
    w2 = -0.5 * a2 * b
    pos = v > 0.0
    return (
        jnp.where(pos, 0.0, w2),
        jnp.where(pos, wm, w1),
        w0,
        jnp.where(pos, w1, wm),
        jnp.where(pos, w2, 0.0),
    )


def split(x):
    hi = x.astype(BF)
    return hi, (x - hi.astype(F32)).astype(BF)


def dot3(a, b, dims):
    ah, al = a
    bh, bl = b
    dn = (dims, ((), ()))
    d = functools.partial(lax.dot_general, dimension_numbers=dn, preferred_element_type=F32)
    return d(ah, bh) + d(al, bh) + d(ah, bl)


def kernel(
    n_y, n_z,
    om_hbm, ve_hbm, own_ref, cell_ref, frac_ref, chord_ref, twist_ref, ang_ref,
    out_hbm, src_out,
    vb, wb, sb, mb, yb, wx, wy, wz, zs, zr, ks, kr, ob,
    vals, sel, pk, p1r, p2s, p2r, p3s, p3r, pvb, srcb, ab,
    ld_sem, ys, yr, zss, zsr, p1s, p1v, p2ss, p2v, p3ss, p3v, ms, mr, kss, ksr, osem,
):
    gy = lax.axis_index("gy")
    gz = lax.axis_index("gz")
    CY, CZ, NX = om_hbm.shape[1], om_hbm.shape[2], om_hbm.shape[3]
    span = n_y // TURBINES
    nvb = max(n_z // 2, 1)
    vb0 = (n_z - nvb) // 2
    NS = span * TURBINES
    zc = gy // 8
    plane = gy % 8
    t_own = jnp.minimum(gy // span, TURBINES - 1)
    rb = (3 * t_own) // 2
    n_zc = n_y // 8
    has_dn, has_up = gy > 0, gy < n_y - 1
    has_l, has_r = gz > 0, gz < n_z - 1
    in_span = gy < NS
    is_src = in_span & (gz >= vb0) & (gz < vb0 + nvb)

    bar = pltpu.get_barrier_semaphore()
    for d in range(1, n_z):
        pl.semaphore_signal(bar, inc=1, device_id=(gy, lax.rem(gz + d, n_z)), device_id_type=MESH)
    for d in range(1, 8):
        pl.semaphore_signal(
            bar, inc=1, device_id=(zc * 8 + lax.rem(plane + d, 8), gz), device_id_type=MESH)
    for d in range(1, n_zc):
        pl.semaphore_signal(
            bar, inc=1, device_id=(lax.rem(zc + d, n_zc) * 8 + plane, gz), device_id_type=MESH)
    n_bar = (n_z - 1) + 7 + (n_zc - 1)
    cross_dn = has_dn & (plane == 0)
    cross_up = has_up & (plane == 7)

    @pl.when(cross_dn)
    def _():
        pl.semaphore_signal(bar, inc=1, device_id=(gy - 1, gz), device_id_type=MESH)

    @pl.when(cross_up)
    def _():
        pl.semaphore_signal(bar, inc=1, device_id=(gy + 1, gz), device_id_type=MESH)

    loads = []
    for c in range(3):
        loads.append(pltpu.make_async_copy(
            ve_hbm.at[c], vb.at[c, pl.ds(2, CY), pl.ds(8, CZ)], ld_sem.at[c]))
        loads.append(pltpu.make_async_copy(
            om_hbm.at[c], wb.at[c, pl.ds(2, CY), pl.ds(8, CZ)], ld_sem.at[3 + c]))
    for cp in loads:
        cp.start()

    ztile = jnp.zeros((8, NX), F32)

    def zfill(i, carry):
        for c in range(3):
            for buf in (vb, wb):
                buf[c, i + 2, pl.ds(0, 8), :] = ztile
                buf[c, i + 2, pl.ds(8 + CZ, 8), :] = ztile
            yb[c, i, pl.ds(0, 8), :] = ztile
            yb[c, i, pl.ds(8 + CZ, 8), :] = ztile
        return carry

    lax.fori_loop(0, CY, zfill, 0)

    def zero_y(lo):
        zrow = jnp.zeros((CZ, NX), F32)
        for c in range(3):
            for k in range(2):
                vb[c, lo + k, pl.ds(8, CZ), :] = zrow
                wb[c, lo + k, pl.ds(8, CZ), :] = zrow
                mb[c, lo + k] = zrow

    @pl.when(jnp.logical_not(has_dn))
    def _():
        zero_y(0)

    @pl.when(jnp.logical_not(has_up))
    def _():
        zero_y(CY + 2)

    @pl.when((zc + 1) * 8 > NS)
    def _():
        for s in range(8):
            @pl.when(zc * 8 + s >= NS)
            def _():
                p2r[s] = ztile

    vals[0:3, :] = cell_ref[...].astype(F32)
    vals[3:6, :] = frac_ref[...]
    my_block = gy * n_z + gz
    row8 = lax.broadcasted_iota(jnp.int32, (8, 128), 0)
    lane = lax.broadcasted_iota(jnp.int32, (8, 128), 1)
    ln128 = lax.broadcasted_iota(jnp.int32, (128, 128), 1)
    sb128 = lax.broadcasted_iota(jnp.int32, (128, 128), 0)
    base0 = pl.multiple_of(rb * 128, 128)
    base1 = pl.multiple_of(rb * 128 + 128, 128)
    o0 = jnp.broadcast_to(own_ref[:, pl.ds(base0, 128)], (8, 128))
    o1 = jnp.broadcast_to(own_ref[:, pl.ds(base1, 128)], (8, 128))
    own = jnp.where(row8 == 0, o0, jnp.where(row8 == 1, o1, -1))
    mine = own == my_block
    mf = mine.astype(F32)
    upper = (sb128 <= ln128).astype(F32)
    csum = jnp.dot(mf, upper, preferred_element_type=F32)
    tot0 = jnp.broadcast_to(csum[0:1, 127:128], (8, 128))
    rank = csum - mf + jnp.where(row8 == 1, tot0, 0.0)
    rank = jnp.where(mine, rank, -1.0)
    rank_t = jnp.transpose(jnp.concatenate([rank] * 16, axis=0))
    lanef = ln128.astype(F32)
    s0 = (jnp.broadcast_to(rank_t[:, 0:1], (128, 128)) == lanef).astype(F32)
    s1 = (jnp.broadcast_to(rank_t[:, 1:2], (128, 128)) == lanef).astype(F32)
    par = jnp.dot(vals[:, pl.ds(base0, 128)], s0, precision=HI, preferred_element_type=F32)
    par = par + jnp.dot(vals[:, pl.ds(base1, 128)], s1, precision=HI, preferred_element_type=F32)
    sel[0] = s0
    sel[1] = s1

    def table(n, k):
        rows = lax.broadcasted_iota(jnp.int32, (n, 128), 0).astype(F32)
        return m4((rows - par[k:k + 1, :]) - par[3 + k:4 + k, :])

    tx = table(NX, 0)
    tyq = table(CY, 1)
    tzq = table(CZ, 2)
    txs = split(tx)

    for cp in loads:
        cp.wait()

    def pack(i, carry):
        c = i // 4
        g = i % 4
        for f, buf in ((0, vb), (1, wb)):
            for j in range(4):
                y = 2 + 4 * g + j
                zs[0, f, c, g, 2 * j:2 * j + 2, :] = buf[c, y, 6 + CZ:8 + CZ, :]
                zs[1, f, c, g, 2 * j:2 * j + 2, :] = buf[c, y, 8:10, :]
        return carry

    lax.fori_loop(0, 12, pack, 0)

    pl.semaphore_wait(bar, n_bar + cross_dn.astype(jnp.int32) + cross_up.astype(jnp.int32))

    def rcopy(src, dst, ss, rs, dev):
        return pltpu.make_async_remote_copy(
            src_ref=src, dst_ref=dst, send_sem=ss, recv_sem=rs, device_id=dev, device_id_type=MESH)

    def z_copy(d):
        return rcopy(zs.at[d], zr.at[d], zss.at[d], zsr.at[d], (gy, gz + (1 if d == 0 else -1)))

    def y_copy(f, d):
        buf = vb if f == 0 else wb
        src, dst = (CY, 0) if d == 0 else (2, CY + 2)
        return rcopy(
            buf.at[:, pl.ds(src, 2), pl.ds(8, CZ)], buf.at[:, pl.ds(dst, 2), pl.ds(8, CZ)],
            ys.at[f, d], yr.at[f, d], (gy + (1 if d == 0 else -1), gz))

    up_cond = ((has_up, has_dn), (has_dn, has_up))
    rt_cond = ((has_r, has_l), (has_l, has_r))
    for d in range(2):
        @pl.when(rt_cond[d][0])
        def _():
            z_copy(d).start()

    for f in range(2):
        for d in range(2):
            @pl.when(up_cond[d][0])
            def _():
                y_copy(f, d).start()

    def sample(y, acc):
        wyr = tyq_row(y)
        out = []
        for c in range(3):
            v = split(vb[c, y + 2, pl.ds(8, CZ), :])
            col = dot3(v, txs, ((1,), (0,))) * tzq
            s = jnp.sum(col, axis=0, keepdims=True)
            out.append(acc[c] + s * wyr)
        return tuple(out)

    ab[0] = tyq

    def tyq_row(y):
        return ab[0, pl.ds(y, 1), :]

    zrow1 = jnp.zeros((1, 128), F32)
    pvq = lax.fori_loop(0, CY, sample, (zrow1, zrow1, zrow1))
    qa = jnp.zeros((8, 128), F32)
    qb = qa
    for c in range(3):
        full = jnp.broadcast_to(pvq[c], (8, 128))
        qa = jnp.where(row8 == c, full, qa)
        qb = jnp.where(row8 == c + 4, full, qb)
    dnt = (((1,), (1,)), ((), ()))
    packet = lax.dot_general(qa, s0, dnt, precision=HI, preferred_element_type=F32)
    packet = packet + lax.dot_general(qb, s1, dnt, precision=HI, preferred_element_type=F32)

    def p1_copy(d):
        return rcopy(pk, p1r.at[gz - vb0], p1s.at[d - 1], p1v.at[gz - vb0],
                     (gy, lax.rem(gz + d, n_z)))

    @pl.when(is_src)
    def _():
        pk[...] = packet
        p1r[gz - vb0] = packet
        for d in range(1, n_z):
            p1_copy(d).start()

    lanes = lax.broadcasted_iota(jnp.int32, (CHUNK, NX), 1)

    def wx_loop(y, carry):
        for z0 in range(0, CZ, CHUNK):
            w = remesh_weights(vb[0, y + 2, pl.ds(8 + z0, CHUNK), :])
            for k in range(5):
                s = k - 2
                x = w[k]
                if s > 0:
                    x = jnp.where(lanes < NX - s, x, 0.0)
                elif s < 0:
                    x = jnp.where(lanes >= -s, x, 0.0)
                wx[k, y, pl.ds(z0, CHUNK), :] = x
        return carry

    lax.fori_loop(0, CY, wx_loop, 0)

    def p1_wait(s):
        return rcopy(p1r.at[s], p1r.at[s], p1s.at[0], p1v.at[s], (gy, gz))

    @pl.when(in_span)
    def _():
        for s in range(nvb):
            @pl.when(gz != vb0 + s)
            def _():
                p1_wait(s).wait_recv()
        tile = p1r[0]
        for s in range(1, nvb):
            tile = tile + p1r[s]
        p2s[...] = tile
        p2r[plane] = tile

    def p2_copy(d):
        return rcopy(p2s, p2r.at[plane], p2ss.at[d - 1], p2v.at[plane],
                     (zc * 8 + lax.rem(plane + d, 8), gz))

    @pl.when(in_span)
    def _():
        for d in range(1, 8):
            p2_copy(d).start()

    def wz_loop(y, carry):
        for z0 in range(0, CZ, CHUNK):
            w = remesh_weights(vb[2, y + 2, pl.ds(8 + z0, CHUNK), :])
            for k in range(5):
                wz[k, y, pl.ds(8 + z0, CHUNK), :] = w[k]
        return carry

    lax.fori_loop(0, CY, wz_loop, 0)

    def wy_one(y):
        for z0 in range(0, CZ, CHUNK):
            w = remesh_weights(vb[1, y, pl.ds(8 + z0, CHUNK), :])
            for k in range(5):
                wy[k, y, pl.ds(z0, CHUNK), :] = w[k]

    def wy_loop(y, carry):
        wy_one(y + 2)
        return carry

    lax.fori_loop(0, CY, wy_loop, 0)

    for s in range(8):
        @pl.when((plane != s) & (zc * 8 + s < NS))
        def _():
            rcopy(p2r.at[s], p2r.at[s], p2ss.at[0], p2v.at[s], (gy, gz)).wait_recv()

    t_a = (zc * 8) // span
    suma = jnp.zeros((8, 128), F32)
    sumb = suma
    for s in range(8):
        x = p2r[s]
        first = (zc * 8 + s) // span == t_a
        suma = suma + jnp.where(first, x, 0.0)
        sumb = sumb + jnp.where(first, 0.0, x)
    p3s[0] = suma
    p3s[1] = sumb
    p3r[zc, 0] = suma
    p3r[zc, 1] = sumb

    def p3_copy(d):
        return rcopy(p3s, p3r.at[zc], p3ss.at[d - 1], p3v.at[zc],
                     (lax.rem(zc + d, n_zc) * 8 + plane, gz))

    for d in range(1, n_zc):
        p3_copy(d).start()

    for d in range(2):
        @pl.when(rt_cond[d][1])
        def _():
            z_copy(d).wait_recv()
            lo = 6 if d == 0 else 8 + CZ

            def unpack(i, carry):
                c = i // 4
                g = i % 4
                for f, buf in ((0, vb), (1, wb)):
                    for j in range(4):
                        buf[c, 2 + 4 * g + j, lo:lo + 2, :] = zr[d, f, c, g, 2 * j:2 * j + 2, :]
                return carry

            lax.fori_loop(0, 12, unpack, 0)

    def wz_edge(y, carry):
        for r0 in (0, 8 + CZ):
            w = remesh_weights(vb[2, y + 2, pl.ds(r0, 8), :])
            for k in range(5):
                wz[k, y, pl.ds(r0, 8), :] = w[k]
        return carry

    lax.fori_loop(0, CY, wz_edge, 0)

    for f in range(2):
        for d in range(2):
            @pl.when(up_cond[d][1])
            def _():
                y_copy(f, d).wait_recv()

    for y in (0, 1, CY + 2, CY + 3):
        wy_one(y)

    c0 = section_step / 12.0
    cl = section_step * viscosity / 12.0

    def around(buf, c, y, z0, dim):
        if dim == 2:
            return [buf[c, y + 2 + k, pl.ds(8 + z0, CHUNK), :] for k in (-2, -1, 1, 2)]
        if dim == 1:
            return [buf[c, y + 2, pl.ds(8 + z0 + k, CHUNK), :] for k in (-2, -1, 1, 2)]
        f = buf[c, y + 2, pl.ds(8 + z0, CHUNK), :]
        res = []
        for k in (-2, -1, 1, 2):
            r = pltpu.roll(f, (-k) % NX, 1)
            m = lanes >= -k if k < 0 else lanes < NX - k
            res.append(jnp.where(m, r, 0.0))
        return res

    def section_loop(y, carry):
        for z0 in range(0, CZ, CHUNK):
            om = [wb[c, y + 2, pl.ds(8 + z0, CHUNK), :] for c in range(3)]
            oms = [c0 * o for o in om]
            for c in range(3):
                acc = om[c]
                near = None
                far = None
                for dim in range(3):
                    a = around(vb, c, y, z0, dim)
                    acc = acc + oms[2 - dim] * (8.0 * (a[2] - a[1]) - (a[3] - a[0]))
                    b = around(wb, c, y, z0, dim)
                    n = b[1] + b[2]
                    e = b[0] + b[3]
                    near = n if near is None else near + n
                    far = e if far is None else far + e
                acc = acc + cl * (16.0 * near - far - 90.0 * om[c])
                sb[c, y, pl.ds(z0, CHUNK), :] = acc
        return carry

    lax.fori_loop(0, CY, section_loop, 0)

    for s in range(n_zc):
        @pl.when(zc != s)
        def _():
            rcopy(p3r.at[s], p3r.at[s], p3ss.at[0], p3v.at[s], (gy, gz)).wait_recv()

    tiles = [jnp.zeros((8, 128), F32) for _ in range(TURBINES)]
    for s in range(n_zc):
        ta = (s * 8) // span
        if ta < TURBINES:
            tiles[ta] = tiles[ta] + p3r[s, 0]
        if ta + 1 < TURBINES:
            tiles[ta + 1] = tiles[ta + 1] + p3r[s, 1]
    for u in range(TURBINES // 2):
        e, o = tiles[2 * u], tiles[2 * u + 1]
        for c in range(3):
            pvb[c, 3 * u:3 * u + 1, :] = e[c:c + 1]
            pvb[c, 3 * u + 1:3 * u + 2, :] = e[4 + c:5 + c] + o[c:c + 1]
            pvb[c, 3 * u + 2:3 * u + 3, :] = o[4 + c:5 + c]
    n_rows = TURBINES * BLADES * BP // 128
    for r in range(n_rows):
        pvb[3, r:r + 1, :] = chord_ref[:, 128 * r:128 * r + 128]
        pvb[4, r:r + 1, :] = twist_ref[:, 128 * r:128 * r + 128]
    r16 = lax.broadcasted_iota(jnp.int32, (16, 128), 0)
    l16 = lax.broadcasted_iota(jnp.int32, (16, 128), 1)
    live = r16 < n_rows
    station = l16 % BP
    blade = (2 * r16 + l16 // BP) % BLADES
    theta = ang_ref[0].astype(F32) * turn_step + 2.0 * 3.141592653589793 / 3.0 * blade.astype(F32)
    radius = (station.astype(F32) + 0.5) / BP
    cos_t = jnp.cos(theta)
    sin_t = jnp.sin(theta)
    chord = jnp.where(live, pvb[3], 0.0)
    twist = jnp.where(live, pvb[4], 0.0)
    rel_x = jnp.where(live, pvb[0], 0.0)
    rel_y = jnp.where(live, pvb[1], 0.0) + tip_speed * radius * sin_t
    rel_z = jnp.where(live, pvb[2], 0.0) - tip_speed * radius * cos_t
    rel_t = -sin_t * rel_y + cos_t * rel_z
    speed = jnp.sqrt(rel_x * rel_x + rel_t * rel_t + 1.0)
    gamma = 3.141592653589793 * chord * (rel_x * jnp.cos(twist) + rel_t * jnp.sin(twist))
    before = jnp.where(station == 0, 0.0, pltpu.roll(gamma, 1, 1))
    ratio = (gamma - before) / speed
    src = [ratio * rel_x, gamma * cos_t + ratio * rel_y, gamma * sin_t + ratio * rel_z]
    for r in range(n_rows):
        srcb[r, 3:8, :] = jnp.zeros((5, 128), F32)
        for c in range(3):
            src_out[c:c + 1, 128 * r:128 * r + 128] = src[c][r:r + 1]
            srcb[r, c:c + 1, :] = src[c][r:r + 1]
    srcq = jnp.dot(srcb[rb], sel[0], precision=HI, preferred_element_type=F32)
    srcq = srcq + jnp.dot(srcb[rb + 1], sel[1], precision=HI, preferred_element_type=F32)
    tyq2 = ab[0]
    for c in range(3):
        ab[c + 1] = section_step * tyq2 * srcq[c:c + 1, :]

    def move_x(y):
        for c in range(3):
            lhs = split(tzq * ab[c + 1, pl.ds(y, 1), :])
            smear = dot3(lhs, txs, ((1,), (1,)))
            f_all = sb[c, y] + smear
            for z0 in range(0, CZ, CHUNK):
                f = f_all[z0:z0 + CHUNK]
                g = wx[2, y, pl.ds(z0, CHUNK), :] * f
                for k in (0, 1, 3, 4):
                    p = wx[k, y, pl.ds(z0, CHUNK), :] * f
                    g = g + pltpu.roll(p, (k - 2) % NX, 1)
                mb[c, y + 2, pl.ds(z0, CHUNK), :] = g

    def edge_loop(i, carry):
        move_x(jnp.where(i < 2, i, i + CY - 4))
        return carry

    lax.fori_loop(0, 4, edge_loop, 0)

    def m_copy(d):
        src_y, dst_y = (CY, 0) if d == 0 else (2, CY + 2)
        return rcopy(mb.at[:, pl.ds(src_y, 2)], mb.at[:, pl.ds(dst_y, 2)],
                     ms.at[d], mr.at[d], (gy + (1 if d == 0 else -1), gz))

    for d in range(2):
        @pl.when(up_cond[d][0])
        def _():
            m_copy(d).start()

    def mid_loop(i, carry):
        move_x(i + 2)
        return carry

    lax.fori_loop(0, CY - 4, mid_loop, 0)

    def move_y(y):
        for z0 in range(0, CZ, CHUNK):
            w = [wy[k, y + 4 - k, pl.ds(z0, CHUNK), :] for k in range(5)]
            for c in range(3):
                g = w[0] * mb[c, y + 4, pl.ds(z0, CHUNK), :]
                for k in range(1, 5):
                    g = g + w[k] * mb[c, y + 4 - k, pl.ds(z0, CHUNK), :]
                yb[c, y, pl.ds(8 + z0, CHUNK), :] = g

    def mid_y(i, carry):
        move_y(i + 2)
        return carry

    lax.fori_loop(0, CY - 4, mid_y, 0)
    for d in range(2):
        @pl.when(up_cond[d][1])
        def _():
            m_copy(d).wait_recv()

    def edge_y(i, carry):
        move_y(jnp.where(i < 2, i, i + CY - 4))
        return carry

    lax.fori_loop(0, 4, edge_y, 0)

    def pack2(i, carry):
        c = i // 4
        g = i % 4
        for j in range(4):
            y = 4 * g + j
            ks[0, c, g, 2 * j:2 * j + 2, :] = yb[c, y, 6 + CZ:8 + CZ, :]
            ks[1, c, g, 2 * j:2 * j + 2, :] = yb[c, y, 8:10, :]
        return carry

    lax.fori_loop(0, 12, pack2, 0)

    def k_copy(d):
        return rcopy(ks.at[d], kr.at[d], kss.at[d], ksr.at[d], (gy, gz + (1 if d == 0 else -1)))

    for d in range(2):
        @pl.when(rt_cond[d][0])
        def _():
            k_copy(d).start()
    for d in range(2):
        @pl.when(rt_cond[d][1])
        def _():
            k_copy(d).wait_recv()
            lo = 6 if d == 0 else 8 + CZ

            def unpack2(i, carry):
                c = i // 4
                g = i % 4
                for j in range(4):
                    yb[c, 4 * g + j, lo:lo + 2, :] = kr[d, c, g, 2 * j:2 * j + 2, :]
                return carry

            lax.fori_loop(0, 12, unpack2, 0)

    def move_z(y, carry):
        for z0 in range(0, CZ, CHUNK):
            w = [wz[k, y, pl.ds(8 + z0 + 2 - k, CHUNK), :] for k in range(5)]
            for c in range(3):
                g = w[0] * yb[c, y, pl.ds(8 + z0 + 2, CHUNK), :]
                for k in range(1, 5):
                    g = g + w[k] * yb[c, y, pl.ds(8 + z0 + 2 - k, CHUNK), :]
                ob[c, y, pl.ds(z0, CHUNK), :] = g
        return carry

    lax.fori_loop(0, CY, move_z, 0)
    oc = pltpu.make_async_copy(ob, out_hbm, osem)
    oc.start()

    for d in range(2):
        @pl.when(rt_cond[d][0])
        def _():
            z_copy(d).wait_send()
            k_copy(d).wait_send()

        @pl.when(up_cond[d][0])
        def _():
            y_copy(0, d).wait_send()
            y_copy(1, d).wait_send()
            m_copy(d).wait_send()

    @pl.when(is_src)
    def _():
        for d in range(1, n_z):
            p1_copy(d).wait_send()

    @pl.when(in_span)
    def _():
        for d in range(1, 8):
            p2_copy(d).wait_send()

    for d in range(1, n_zc):
        p3_copy(d).wait_send()
    oc.wait()


def on_device(n_y, n_z, omega, velocity, owner, cells, frac, chord, twist, angle):
    _, cy, cz, nx = omega.shape
    n_p = owner.shape[0]
    n_zc = n_y // 8
    vm = pl.BlockSpec(memory_space=pltpu.VMEM)
    hb = pl.BlockSpec(memory_space=pl.ANY)
    sm = pl.BlockSpec(memory_space=pltpu.SMEM)
    nvb = max(n_z // 2, 1)
    V = pltpu.VMEM
    D = pltpu.SemaphoreType.DMA
    scratch = [
        V((3, cy + 4, cz + 16, nx), F32),
        V((3, cy + 4, cz + 16, nx), F32),
        V((3, cy, cz, nx), F32),
        V((3, cy + 4, cz, nx), F32),
        V((3, cy, cz + 16, nx), F32),
        V((5, cy, cz, nx), F32),
        V((5, cy + 4, cz, nx), F32),
        V((5, cy, cz + 16, nx), F32),
        V((2, 2, 3, cy // 4, 8, nx), F32),
        V((2, 2, 3, cy // 4, 8, nx), F32),
        V((2, 3, cy // 4, 8, nx), F32),
        V((2, 3, cy // 4, 8, nx), F32),
        V((3, cy, cz, nx), F32),
        V((8, n_p), F32),
        V((2, 128, 128), F32),
        V((8, 128), F32),
        V((nvb, 8, 128), F32),
        V((8, 128), F32),
        V((8, 8, 128), F32),
        V((2, 8, 128), F32),
        V((n_zc, 2, 8, 128), F32),
        V((5, 16, 128), F32),
        V((n_p // 128, 8, 128), F32),
        V((4, cy, 128), F32),
        D((6,)), D((2, 2)), D((2, 2)), D((2,)), D((2,)),
        D((n_z - 1,)), D((nvb,)), D((7,)), D((8,)), D((n_zc - 1,)), D((n_zc,)),
        D((2,)), D((2,)), D((2,)), D((2,)), D(()),
    ]
    out, src = pl.pallas_call(
        functools.partial(kernel, n_y, n_z),
        name="section",
        out_shape=(
            jax.ShapeDtypeStruct(omega.shape, F32),
            jax.ShapeDtypeStruct((3, n_p), F32),
        ),
        in_specs=[hb, hb, vm, vm, vm, vm, vm, sm],
        out_specs=(hb, vm),
        scratch_shapes=scratch,
        compiler_params=pltpu.CompilerParams(
            collective_id=0, has_side_effects=True, vmem_limit_bytes=60 * 1024 * 1024),
    )(omega, velocity, owner.reshape(1, n_p), cells, frac,
      chord.reshape(1, n_p), twist.reshape(1, n_p), angle)
    return out, src


def solution(mesh):
    n_y, n_z = mesh.shape["gy"], mesh.shape["gz"]
    field = P(None, "gy", "gz", None)
    return jax.shard_map(
        functools.partial(on_device, n_y, n_z),
        mesh=mesh,
        in_specs=(field, field, P(), P(), P(), P(), P(), P()),
        out_specs=(field, P()),
        check_vma=False,
    )
```

```python
import functools

import jax
import jax.numpy as jnp
from jax import lax
from jax.experimental import pallas as pl
from jax.experimental.pallas import tpu as pltpu
from jax.sharding import PartitionSpec as P

TURBINES = 6
BLADES = 3
BP = 64
MESH = pl.DeviceIdType.MESH
HI = lax.Precision.HIGHEST

section_step = 0.4
viscosity = 0.05
tip_speed = 3.0
turn_step = 2.0 * 3.141592653589793 / 720.0
F32 = jnp.float32
BF = jnp.bfloat16

CHUNK = 32


def m4(shift):
    mag = jnp.abs(shift)
    inner = 1.0 + mag * mag * (1.5 * mag - 2.5)
    far = 2.0 - mag
    outer = 0.5 * far * far * (1.0 - mag)
    return jnp.where(mag < 1.0, inner, jnp.where(mag < 2.0, outer, 0.0))


def remesh_weights(v):
    a = jnp.minimum(section_step * jnp.abs(v), 1.0)
    b = 1.0 - a
    a2 = a * a
    b2 = b * b
    w0 = 1.0 + a2 * (1.5 * a - 2.5)
    w1 = 1.0 + b2 * (1.5 * b - 2.5)
    wm = -0.5 * a * b2
    w2 = -0.5 * a2 * b
    pos = v > 0.0
    return (
        jnp.where(pos, 0.0, w2),
        jnp.where(pos, wm, w1),
        w0,
        jnp.where(pos, w1, wm),
        jnp.where(pos, w2, 0.0),
    )


def split(x):
    hi = x.astype(BF)
    return hi, (x - hi.astype(F32)).astype(BF)


def dot3(a, b, dims):
    ah, al = a
    bh, bl = b
    dn = (dims, ((), ()))
    d = functools.partial(lax.dot_general, dimension_numbers=dn, preferred_element_type=F32)
    return d(ah, bh) + d(al, bh) + d(ah, bl)


def kernel(
    n_y, n_z,
    om_hbm, ve_hbm, own_ref, cell_ref, frac_ref, chord_ref, twist_ref, ang_ref,
    out_ref, src_out,
    vb, wb, sb, mb, yb, wx, wy, wz, zs, zr, ks, kr,
    vals, sel, pk, p1r, p2s, p2r, p3s, p3r, pvb, tall, ab,
    ld_sem, ys, yr, zss, zsr, p1s, p1v, p2ss, p2v, p3ss, p3v, ms, mr, kss, ksr,
):
    gy = lax.axis_index("gy")
    gz = lax.axis_index("gz")
    CY, CZ, NX = om_hbm.shape[1], om_hbm.shape[2], om_hbm.shape[3]
    span = n_y // TURBINES
    nvb = max(n_z // 2, 1)
    vb0 = (n_z - nvb) // 2
    NS = span * TURBINES
    zc = gy // 8
    plane = gy % 8
    t_own = jnp.minimum(gy // span, TURBINES - 1)
    rb = (3 * t_own) // 2
    n_zc = n_y // 8
    has_dn, has_up = gy > 0, gy < n_y - 1
    has_l, has_r = gz > 0, gz < n_z - 1
    in_span = gy < NS
    is_src = in_span & (gz >= vb0) & (gz < vb0 + nvb)
    place = gy % span

    def peer(d):
        return t_own * span + lax.rem(place + d, span)


    bar = pltpu.get_barrier_semaphore()
    for d in range(1, n_z):
        pl.semaphore_signal(bar, inc=1, device_id=(gy, lax.rem(gz + d, n_z)), device_id_type=MESH)
    for d in range(1, n_zc):
        pl.semaphore_signal(
            bar, inc=1, device_id=(lax.rem(zc + d, n_zc) * 8 + plane, gz), device_id_type=MESH)

    @pl.when(in_span)
    def _():
        for d in range(1, span):
            pl.semaphore_signal(bar, inc=1, device_id=(peer(d), gz), device_id_type=MESH)

    loose = jnp.logical_not(in_span)
    cross_dn = has_dn & ((place == 0) | loose)
    cross_up = has_up & ((place == span - 1) | loose)
    n_bar = (
        (n_z - 1) + (n_zc - 1) + jnp.where(in_span, span - 1, 0)
        + cross_dn.astype(jnp.int32) + cross_up.astype(jnp.int32))

    @pl.when(cross_dn)
    def _():
        pl.semaphore_signal(bar, inc=1, device_id=(gy - 1, gz), device_id_type=MESH)

    @pl.when(cross_up)
    def _():
        pl.semaphore_signal(bar, inc=1, device_id=(gy + 1, gz), device_id_type=MESH)

    loads = []
    for c in range(3):
        loads.append(pltpu.make_async_copy(
            ve_hbm.at[c], vb.at[c, pl.ds(2, CY), pl.ds(8, CZ)], ld_sem.at[c]))
        loads.append(pltpu.make_async_copy(
            om_hbm.at[c], wb.at[c, pl.ds(2, CY), pl.ds(8, CZ)], ld_sem.at[3 + c]))
    for cp in loads:
        cp.start()

    ztile = jnp.zeros((8, NX), F32)

    def zfill(i, carry):
        for c in range(3):
            for buf in (vb, wb):
                buf[c, i + 2, pl.ds(0, 8), :] = ztile
                buf[c, i + 2, pl.ds(8 + CZ, 8), :] = ztile
            yb[c, i, pl.ds(0, 8), :] = ztile
            yb[c, i, pl.ds(8 + CZ, 8), :] = ztile
        return carry

    lax.fori_loop(0, CY, zfill, 0)

    def zero_y(lo):
        zrow = jnp.zeros((CZ, NX), F32)
        for c in range(3):
            for k in range(2):
                vb[c, lo + k, pl.ds(8, CZ), :] = zrow
                wb[c, lo + k, pl.ds(8, CZ), :] = zrow
                mb[c, lo + k] = zrow

    @pl.when(jnp.logical_not(has_dn))
    def _():
        zero_y(0)

    @pl.when(jnp.logical_not(has_up))
    def _():
        zero_y(CY + 2)

    vals[0:3, :] = cell_ref[...].astype(F32)
    vals[3:6, :] = frac_ref[...]
    my_block = gy * n_z + gz
    row8 = lax.broadcasted_iota(jnp.int32, (8, 128), 0)
    lane = lax.broadcasted_iota(jnp.int32, (8, 128), 1)
    ln128 = lax.broadcasted_iota(jnp.int32, (128, 128), 1)
    sb128 = lax.broadcasted_iota(jnp.int32, (128, 128), 0)
    base0 = pl.multiple_of(rb * 128, 128)
    base1 = pl.multiple_of(rb * 128 + 128, 128)
    o0 = jnp.broadcast_to(own_ref[pl.ds(base0, 128)].reshape(1, 128), (8, 128))
    o1 = jnp.broadcast_to(own_ref[pl.ds(base1, 128)].reshape(1, 128), (8, 128))
    own = jnp.where(row8 == 0, o0, jnp.where(row8 == 1, o1, -1))
    mine = own == my_block
    mf = mine.astype(F32)
    upper = (sb128 <= ln128).astype(F32)
    csum = jnp.dot(mf, upper, preferred_element_type=F32)
    tot0 = jnp.broadcast_to(csum[0:1, 127:128], (8, 128))
    rank = csum - mf + jnp.where(row8 == 1, tot0, 0.0)
    rank = jnp.where(mine, rank, -1.0)
    rank_t = jnp.transpose(jnp.concatenate([rank] * 16, axis=0))
    lanef = ln128.astype(F32)
    s0 = (jnp.broadcast_to(rank_t[:, 0:1], (128, 128)) == lanef).astype(F32)
    s1 = (jnp.broadcast_to(rank_t[:, 1:2], (128, 128)) == lanef).astype(F32)
    par = jnp.dot(vals[:, pl.ds(base0, 128)], s0, precision=HI, preferred_element_type=F32)
    par = par + jnp.dot(vals[:, pl.ds(base1, 128)], s1, precision=HI, preferred_element_type=F32)
    sel[0] = s0
    sel[1] = s1

    def table(n, k):
        rows = lax.broadcasted_iota(jnp.int32, (n, 128), 0).astype(F32)
        return m4((rows - par[k:k + 1, :]) - par[3 + k:4 + k, :])

    tx = table(NX, 0)
    tyq = table(CY, 1)
    tzq = table(CZ, 2)
    txs = split(tx)

    for cp in loads:
        cp.wait()

    def pack(i, carry):
        c = i // 4
        g = i % 4
        for f, buf in ((0, vb), (1, wb)):
            for j in range(4):
                y = 2 + 4 * g + j
                zs[0, f, c, g, 2 * j:2 * j + 2, :] = buf[c, y, 6 + CZ:8 + CZ, :]
                zs[1, f, c, g, 2 * j:2 * j + 2, :] = buf[c, y, 8:10, :]
        return carry

    lax.fori_loop(0, 12, pack, 0)

    def sample(y, acc):
        wyr = tyq_row(y)
        out = []
        for c in range(3):
            v = split(vb[c, y + 2, pl.ds(8, CZ), :])
            col = dot3(v, txs, ((1,), (0,))) * tzq
            s = jnp.sum(col, axis=0, keepdims=True)
            out.append(acc[c] + s * wyr)
        return tuple(out)

    ab[0] = tyq

    def tyq_row(y):
        return ab[0, pl.ds(y, 1), :]

    zrow1 = jnp.zeros((1, 128), F32)
    pvq = lax.fori_loop(0, CY, sample, (zrow1, zrow1, zrow1))
    qa = jnp.zeros((8, 128), F32)
    qb = qa
    for c in range(3):
        full = jnp.broadcast_to(pvq[c], (8, 128))
        qa = jnp.where(row8 == c, full, qa)
        qb = jnp.where(row8 == c + 4, full, qb)
    dnt = (((1,), (1,)), ((), ()))
    packet = lax.dot_general(qa, s0, dnt, precision=HI, preferred_element_type=F32)
    packet = packet + lax.dot_general(qb, s1, dnt, precision=HI, preferred_element_type=F32)

    def trig(rows, twist):
        col = lax.broadcasted_iota(jnp.int32, rows.shape, 1)
        station = col % BP
        blade = (2 * rows + col // BP) % BLADES
        theta = ang_ref[0].astype(F32) * turn_step
        theta = theta + 2.0 * 3.141592653589793 / 3.0 * blade.astype(F32)
        radius = (station.astype(F32) + 0.5) / BP
        return station, tip_speed * radius, jnp.cos(theta), jnp.sin(theta), jnp.cos(twist), jnp.sin(twist)

    def forces(angles, chord, pv):
        station, reach, cos_t, sin_t, cos_w, sin_w = angles
        rel_x = pv[0]
        rel_y = pv[1] + reach * sin_t
        rel_z = pv[2] - reach * cos_t
        rel_t = -sin_t * rel_y + cos_t * rel_z
        speed = jnp.sqrt(rel_x * rel_x + rel_t * rel_t + 1.0)
        gamma = 3.141592653589793 * chord * (rel_x * cos_w + rel_t * sin_w)
        before = jnp.where(station == 0, 0.0, pltpu.roll(gamma, 1, 1))
        ratio = (gamma - before) / speed
        return [ratio * rel_x, gamma * cos_t + ratio * rel_y, gamma * sin_t + ratio * rel_z]

    def pick(a, b):
        a, b = jnp.broadcast_to(a, (8, 128)), jnp.broadcast_to(b, (8, 128))
        return jnp.where(row8 == 0, a, jnp.where(row8 == 1, b, 0.0))

    def pair(ref):
        return pick(ref[pl.ds(base0, 128)].reshape(1, 128), ref[pl.ds(base1, 128)].reshape(1, 128))

    trig2 = trig(row8 + rb, pair(twist_ref))
    chord2 = pair(chord_ref)

    pl.semaphore_wait(bar, n_bar)

    def rcopy(src, dst, ss, rs, dev):
        return pltpu.make_async_remote_copy(
            src_ref=src, dst_ref=dst, send_sem=ss, recv_sem=rs, device_id=dev, device_id_type=MESH)

    def z_copy(d):
        return rcopy(zs.at[d], zr.at[d], zss.at[d], zsr.at[d], (gy, gz + (1 if d == 0 else -1)))

    def y_copy(f, d):
        buf = vb if f == 0 else wb
        src, dst = (CY, 0) if d == 0 else (2, CY + 2)
        return rcopy(
            buf.at[:, pl.ds(src, 2), pl.ds(8, CZ)], buf.at[:, pl.ds(dst, 2), pl.ds(8, CZ)],
            ys.at[f, d], yr.at[f, d], (gy + (1 if d == 0 else -1), gz))

    def p1_copy(d):
        return rcopy(pk, p1r.at[gz - vb0], p1s.at[d - 1], p1v.at[gz - vb0],
                     (gy, lax.rem(gz + d, n_z)))

    @pl.when(is_src)
    def _():
        pk[...] = packet
        p1r[gz - vb0] = packet
        for d in range(1, n_z):
            p1_copy(d).start()

    up_cond = ((has_up, has_dn), (has_dn, has_up))
    rt_cond = ((has_r, has_l), (has_l, has_r))
    for d in range(2):
        @pl.when(rt_cond[d][0])
        def _():
            z_copy(d).start()

    for f in range(2):
        for d in range(2):
            @pl.when(up_cond[d][0])
            def _():
                y_copy(f, d).start()

    lanes = lax.broadcasted_iota(jnp.int32, (CHUNK, NX), 1)

    def wx_loop(y, carry):
        for z0 in range(0, CZ, CHUNK):
            w = remesh_weights(vb[0, y + 2, pl.ds(8 + z0, CHUNK), :])
            for k in range(5):
                s = k - 2
                x = w[k]
                if s > 0:
                    x = jnp.where(lanes < NX - s, x, 0.0)
                elif s < 0:
                    x = jnp.where(lanes >= -s, x, 0.0)
                wx[k, y, pl.ds(z0, CHUNK), :] = x
        return carry

    lax.fori_loop(0, CY, wx_loop, 0)

    def p1_wait(s):
        return rcopy(p1r.at[s], p1r.at[s], p1s.at[0], p1v.at[s], (gy, gz))

    @pl.when(in_span)
    def _():
        for s in range(nvb):
            @pl.when(gz != vb0 + s)
            def _():
                p1_wait(s).wait_recv()
        tile = p1r[0]
        for s in range(1, nvb):
            tile = tile + p1r[s]
        p2s[...] = tile
        p2r[0] = tile

    def p2_copy(d):
        return rcopy(p2s, p2r.at[d], p2ss.at[d - 1], p2v.at[d], (peer(d), gz))

    @pl.when(in_span)
    def _():
        for d in range(1, span):
            p2_copy(d).start()

    def p3_copy(d):
        return rcopy(p3s, p3r.at[zc], p3ss.at[d - 1], p3v.at[zc],
                     (lax.rem(zc + d, n_zc) * 8 + plane, gz))

    def wz_loop(y, carry):
        for z0 in range(0, CZ, CHUNK):
            w = remesh_weights(vb[2, y + 2, pl.ds(8 + z0, CHUNK), :])
            for k in range(5):
                wz[k, y, pl.ds(8 + z0, CHUNK), :] = w[k]
        return carry

    lax.fori_loop(0, CY, wz_loop, 0)

    def wy_one(y):
        for z0 in range(0, CZ, CHUNK):
            w = remesh_weights(vb[1, y, pl.ds(8 + z0, CHUNK), :])
            for k in range(5):
                wy[k, y, pl.ds(z0, CHUNK), :] = w[k]

    def wy_loop(y, carry):
        wy_one(y + 2)
        return carry

    lax.fori_loop(0, CY, wy_loop, 0)

    for d in range(2):
        @pl.when(rt_cond[d][1])
        def _():
            z_copy(d).wait_recv()
            lo = 6 if d == 0 else 8 + CZ

            def unpack(i, carry):
                c = i // 4
                g = i % 4
                for f, buf in ((0, vb), (1, wb)):
                    for j in range(4):
                        buf[c, 2 + 4 * g + j, lo:lo + 2, :] = zr[d, f, c, g, 2 * j:2 * j + 2, :]
                return carry

            lax.fori_loop(0, 12, unpack, 0)

    def wz_edge(y, carry):
        for r0 in (0, 8 + CZ):
            w = remesh_weights(vb[2, y + 2, pl.ds(r0, 8), :])
            for k in range(5):
                wz[k, y, pl.ds(r0, 8), :] = w[k]
        return carry

    lax.fori_loop(0, CY, wz_edge, 0)

    for f in range(2):
        for d in range(2):
            @pl.when(up_cond[d][1])
            def _():
                y_copy(f, d).wait_recv()

    for y in (0, 1, CY + 2, CY + 3):
        wy_one(y)

    c0 = section_step / 12.0
    cl = section_step * viscosity / 12.0

    def around(buf, c, y, z0, dim):
        if dim == 2:
            return [buf[c, y + 2 + k, pl.ds(8 + z0, CHUNK), :] for k in (-2, -1, 1, 2)]
        if dim == 1:
            return [buf[c, y + 2, pl.ds(8 + z0 + k, CHUNK), :] for k in (-2, -1, 1, 2)]
        f = buf[c, y + 2, pl.ds(8 + z0, CHUNK), :]
        res = []
        for k in (-2, -1, 1, 2):
            r = pltpu.roll(f, (-k) % NX, 1)
            m = lanes >= -k if k < 0 else lanes < NX - k
            res.append(jnp.where(m, r, 0.0))
        return res

    def section_loop(y, carry):
        for z0 in range(0, CZ, CHUNK):
            om = [wb[c, y + 2, pl.ds(8 + z0, CHUNK), :] for c in range(3)]
            oms = [c0 * o for o in om]
            for c in range(3):
                acc = om[c]
                near = None
                far = None
                for dim in range(3):
                    a = around(vb, c, y, z0, dim)
                    acc = acc + oms[2 - dim] * (8.0 * (a[2] - a[1]) - (a[3] - a[0]))
                    b = around(wb, c, y, z0, dim)
                    n = b[1] + b[2]
                    e = b[0] + b[3]
                    near = n if near is None else near + n
                    far = e if far is None else far + e
                acc = acc + cl * (16.0 * near - far - 90.0 * om[c])
                sb[c, y, pl.ds(z0, CHUNK), :] = acc
        return carry

    lax.fori_loop(0, CY, section_loop, 0)

    @pl.when(in_span)
    def _():
        for d in range(1, span):
            rcopy(p2r.at[d], p2r.at[d], p2ss.at[0], p2v.at[d], (gy, gz)).wait_recv()
        tile = p2r[0]
        for d in range(1, span):
            tile = tile + p2r[d]
        p3s[...] = tile
        p3r[zc] = tile
        for d in range(1, n_zc):
            p3_copy(d).start()

    @pl.when(is_src)
    def _():
        tile = p3s[...]
        pv2 = [pick(tile[c:c + 1], tile[4 + c:5 + c]) for c in range(3)]
        src = forces(trig2, chord2, pv2)
        e0 = jnp.zeros((8, 128), F32)
        e1 = e0
        for c in range(3):
            e0 = jnp.where(row8 == c, jnp.broadcast_to(src[c][0:1], (8, 128)), e0)
            e1 = jnp.where(row8 == c, jnp.broadcast_to(src[c][1:2], (8, 128)), e1)
        srcq = jnp.dot(e0, sel[0], precision=HI, preferred_element_type=F32)
        srcq = srcq + jnp.dot(e1, sel[1], precision=HI, preferred_element_type=F32)
        for c in range(3):
            ab[c + 1] = section_step * ab[0] * srcq[c:c + 1, :]

    def move_x(y):
        for c in range(3):
            for z0 in range(0, CZ, CHUNK):
                f = sb[c, y, pl.ds(z0, CHUNK), :]
                g = wx[2, y, pl.ds(z0, CHUNK), :] * f
                for k in (0, 1, 3, 4):
                    p = wx[k, y, pl.ds(z0, CHUNK), :] * f
                    g = g + pltpu.roll(p, (k - 2) % NX, 1)
                mb[c, y + 2, pl.ds(z0, CHUNK), :] = g

    def smear_loop(y, carry):
        for c in range(3):
            lhs = split(tzq * ab[c + 1, pl.ds(y, 1), :])
            sb[c, y] = sb[c, y] + dot3(lhs, txs, ((1,), (1,)))
        return carry

    @pl.when(is_src)
    def _():
        lax.fori_loop(0, CY, smear_loop, 0)

    def edge_loop(i, carry):
        move_x(jnp.where(i < 2, i, i + CY - 4))
        return carry

    lax.fori_loop(0, 4, edge_loop, 0)

    def m_copy(d):
        src_y, dst_y = (CY, 0) if d == 0 else (2, CY + 2)
        return rcopy(mb.at[:, pl.ds(src_y, 2)], mb.at[:, pl.ds(dst_y, 2)],
                     ms.at[d], mr.at[d], (gy + (1 if d == 0 else -1), gz))

    for d in range(2):
        @pl.when(up_cond[d][0])
        def _():
            m_copy(d).start()

    def mid_loop(i, carry):
        move_x(i + 2)
        return carry

    lax.fori_loop(0, CY - 4, mid_loop, 0)

    def move_y(y):
        for z0 in range(0, CZ, CHUNK):
            w = [wy[k, y + 4 - k, pl.ds(z0, CHUNK), :] for k in range(5)]
            for c in range(3):
                g = w[0] * mb[c, y + 4, pl.ds(z0, CHUNK), :]
                for k in range(1, 5):
                    g = g + w[k] * mb[c, y + 4 - k, pl.ds(z0, CHUNK), :]
                yb[c, y, pl.ds(8 + z0, CHUNK), :] = g

    def mid_y(i, carry):
        move_y(i + 2)
        return carry

    lax.fori_loop(0, CY - 4, mid_y, 0)
    for d in range(2):
        @pl.when(up_cond[d][1])
        def _():
            m_copy(d).wait_recv()

    def edge_y(i, carry):
        move_y(jnp.where(i < 2, i, i + CY - 4))
        return carry

    lax.fori_loop(0, 4, edge_y, 0)

    def pack2(i, carry):
        c = i // 4
        g = i % 4
        for j in range(4):
            y = 4 * g + j
            ks[0, c, g, 2 * j:2 * j + 2, :] = yb[c, y, 6 + CZ:8 + CZ, :]
            ks[1, c, g, 2 * j:2 * j + 2, :] = yb[c, y, 8:10, :]
        return carry

    lax.fori_loop(0, 12, pack2, 0)

    def k_copy(d):
        return rcopy(ks.at[d], kr.at[d], kss.at[d], ksr.at[d], (gy, gz + (1 if d == 0 else -1)))

    for d in range(2):
        @pl.when(rt_cond[d][0])
        def _():
            k_copy(d).start()
    for d in range(2):
        @pl.when(rt_cond[d][1])
        def _():
            k_copy(d).wait_recv()
            lo = 6 if d == 0 else 8 + CZ

            def unpack2(i, carry):
                c = i // 4
                g = i % 4
                for j in range(4):
                    yb[c, 4 * g + j, lo:lo + 2, :] = kr[d, c, g, 2 * j:2 * j + 2, :]
                return carry

            lax.fori_loop(0, 12, unpack2, 0)

    def move_z(y, carry):
        for z0 in range(0, CZ, CHUNK):
            w = [wz[k, y, pl.ds(8 + z0 + 2 - k, CHUNK), :] for k in range(5)]
            for c in range(3):
                g = w[0] * yb[c, y, pl.ds(8 + z0 + 2, CHUNK), :]
                for k in range(1, 5):
                    g = g + w[k] * yb[c, y, pl.ds(8 + z0 + 2 - k, CHUNK), :]
                out_ref[c, y, pl.ds(z0, CHUNK), :] = g
        return carry

    lax.fori_loop(0, CY, move_z, 0)

    for s in range(n_zc):
        @pl.when((zc != s) & (s * 8 + plane < NS))
        def _():
            rcopy(p3r.at[s], p3r.at[s], p3ss.at[0], p3v.at[s], (gy, gz)).wait_recv()

    for s in range(n_zc):
        @pl.when(s * 8 + plane < NS)
        def _():
            tall[(s * 8 + plane) // span] = p3r[s]

    for u in range(TURBINES // 2):
        e, o = tall[2 * u], tall[2 * u + 1]
        for c in range(3):
            pvb[c, 3 * u:3 * u + 1, :] = e[c:c + 1]
            pvb[c, 3 * u + 1:3 * u + 2, :] = e[4 + c:5 + c] + o[c:c + 1]
            pvb[c, 3 * u + 2:3 * u + 3, :] = o[4 + c:5 + c]
    n_rows = TURBINES * BLADES * BP // 128
    for r in range(n_rows):
        pvb[3, r:r + 1, :] = chord_ref[128 * r:128 * r + 128].reshape(1, 128)
        pvb[4, r:r + 1, :] = twist_ref[128 * r:128 * r + 128].reshape(1, 128)
    r16 = lax.broadcasted_iota(jnp.int32, (16, 128), 0)
    live = r16 < n_rows
    full = forces(
        trig(r16, jnp.where(live, pvb[4], 0.0)), jnp.where(live, pvb[3], 0.0),
        [jnp.where(live, pvb[c], 0.0) for c in range(3)])
    for r in range(n_rows):
        for c in range(3):
            src_out[c:c + 1, 128 * r:128 * r + 128] = full[c][r:r + 1]

    for d in range(2):
        @pl.when(rt_cond[d][0])
        def _():
            z_copy(d).wait_send()
            k_copy(d).wait_send()

        @pl.when(up_cond[d][0])
        def _():
            y_copy(0, d).wait_send()
            y_copy(1, d).wait_send()
            m_copy(d).wait_send()

    @pl.when(is_src)
    def _():
        for d in range(1, n_z):
            p1_copy(d).wait_send()

    @pl.when(in_span)
    def _():
        for d in range(1, span):
            p2_copy(d).wait_send()
        for d in range(1, n_zc):
            p3_copy(d).wait_send()


def on_device(n_y, n_z, omega, velocity, owner, cells, frac, chord, twist, angle):
    _, cy, cz, nx = omega.shape
    n_p = owner.shape[0]
    n_zc = n_y // 8
    vm = pl.BlockSpec(memory_space=pltpu.VMEM)
    hb = pl.BlockSpec(memory_space=pl.ANY)
    sm = pl.BlockSpec(memory_space=pltpu.SMEM)
    nvb = max(n_z // 2, 1)
    V = pltpu.VMEM
    D = pltpu.SemaphoreType.DMA
    scratch = [
        V((3, cy + 4, cz + 16, nx), F32),
        V((3, cy + 4, cz + 16, nx), F32),
        V((3, cy, cz, nx), F32),
        V((3, cy + 4, cz, nx), F32),
        V((3, cy, cz + 16, nx), F32),
        V((5, cy, cz, nx), F32),
        V((5, cy + 4, cz, nx), F32),
        V((5, cy, cz + 16, nx), F32),
        V((2, 2, 3, cy // 4, 8, nx), F32),
        V((2, 2, 3, cy // 4, 8, nx), F32),
        V((2, 3, cy // 4, 8, nx), F32),
        V((2, 3, cy // 4, 8, nx), F32),
        V((8, n_p), F32),
        V((2, 128, 128), F32),
        V((8, 128), F32),
        V((nvb, 8, 128), F32),
        V((8, 128), F32),
        V((n_y // TURBINES, 8, 128), F32),
        V((8, 128), F32),
        V((n_zc, 8, 128), F32),
        V((5, 16, 128), F32),
        V((TURBINES, 8, 128), F32),
        V((4, cy, 128), F32),
        D((6,)), D((2, 2)), D((2, 2)), D((2,)), D((2,)),
        D((n_z - 1,)), D((nvb,)), D((n_y // TURBINES - 1,)), D((n_y // TURBINES,)), D((n_zc - 1,)), D((n_zc,)),
        D((2,)), D((2,)), D((2,)), D((2,)),
    ]
    out, src = pl.pallas_call(
        functools.partial(kernel, n_y, n_z),
        name="section",
        out_shape=(
            pltpu.VMEM(omega.shape, F32),
            jax.ShapeDtypeStruct((3, n_p), F32),
        ),
        in_specs=[hb, hb, vm, vm, vm, vm, vm, sm],
        out_specs=(vm, vm),
        scratch_shapes=scratch,
        compiler_params=pltpu.CompilerParams(
            collective_id=0, has_side_effects=True, vmem_limit_bytes=60 * 1024 * 1024),
    )(omega, velocity, owner, cells, frac, chord, twist, angle)
    return out, src


def solution(mesh):
    n_y, n_z = mesh.shape["gy"], mesh.shape["gz"]
    field = P(None, "gy", "gz", None)
    return jax.shard_map(
        functools.partial(on_device, n_y, n_z),
        mesh=mesh,
        in_specs=(field, field, P(), P(), P(), P(), P(), P()),
        out_specs=(field, P()),
        check_vma=False,
    )
```

```python
import functools

import jax
import jax.numpy as jnp
from jax import lax
from jax.experimental import pallas as pl
from jax.experimental.pallas import tpu as pltpu
from jax.sharding import PartitionSpec as P

TURBINES = 6
BLADES = 3
BP = 64
MESH = pl.DeviceIdType.MESH
HI = lax.Precision.HIGHEST

section_step = 0.4
viscosity = 0.05
tip_speed = 3.0
turn_step = 2.0 * 3.141592653589793 / 720.0
F32 = jnp.float32
BF = jnp.bfloat16

CHUNK = 32


def m4(shift):
    mag = jnp.abs(shift)
    inner = 1.0 + mag * mag * (1.5 * mag - 2.5)
    far = 2.0 - mag
    outer = 0.5 * far * far * (1.0 - mag)
    return jnp.where(mag < 1.0, inner, jnp.where(mag < 2.0, outer, 0.0))


def remesh_weights(v):
    a = jnp.minimum(section_step * jnp.abs(v), 1.0)
    b = 1.0 - a
    a2 = a * a
    b2 = b * b
    w0 = 1.0 + a2 * (1.5 * a - 2.5)
    w1 = 1.0 + b2 * (1.5 * b - 2.5)
    wm = -0.5 * a * b2
    w2 = -0.5 * a2 * b
    pos = v > 0.0
    return (
        jnp.where(pos, 0.0, w2),
        jnp.where(pos, wm, w1),
        w0,
        jnp.where(pos, w1, wm),
        jnp.where(pos, w2, 0.0),
    )


def split(x):
    hi = x.astype(BF)
    return hi, (x - hi.astype(F32)).astype(BF)


def dot3(a, b, dims):
    ah, al = a
    bh, bl = b
    dn = (dims, ((), ()))
    d = functools.partial(lax.dot_general, dimension_numbers=dn, preferred_element_type=F32)
    return d(ah, bh) + d(al, bh) + d(ah, bl)


def kernel(
    n_y, n_z,
    om_hbm, ve_hbm, own_ref, cell_ref, frac_ref, chord_ref, twist_ref, ang_ref,
    out_ref, src_out,
    vb, wb, sb, mb, yb, wx, wy, wz, zs, zr, ks, kr,
    vals, sel, pk, p1r, p2s, p2r, p3s, p3r, pvb, tall, ab, txb, tzb,
    ld_sem, ys, yr, zss, zsr, p1s, p1v, p2ss, p2v, p3ss, p3v, ms, mr, kss, ksr,
):
    gy = lax.axis_index("gy")
    gz = lax.axis_index("gz")
    CY, CZ, NX = om_hbm.shape[1], om_hbm.shape[2], om_hbm.shape[3]
    span = n_y // TURBINES
    nvb = max(n_z // 2, 1)
    vb0 = (n_z - nvb) // 2
    NS = span * TURBINES
    zc = gy // 8
    plane = gy % 8
    t_own = jnp.minimum(gy // span, TURBINES - 1)
    rb = (3 * t_own) // 2
    n_zc = n_y // 8
    has_dn, has_up = gy > 0, gy < n_y - 1
    has_l, has_r = gz > 0, gz < n_z - 1
    in_span = gy < NS
    is_src = in_span & (gz >= vb0) & (gz < vb0 + nvb)
    place = gy % span

    def peer(d):
        return t_own * span + lax.rem(place + d, span)


    bar = pltpu.get_barrier_semaphore()
    for d in range(1, n_z):
        pl.semaphore_signal(bar, inc=1, device_id=(gy, lax.rem(gz + d, n_z)), device_id_type=MESH)
    for d in range(1, n_zc):
        pl.semaphore_signal(
            bar, inc=1, device_id=(lax.rem(zc + d, n_zc) * 8 + plane, gz), device_id_type=MESH)

    @pl.when(in_span)
    def _():
        for d in range(1, span):
            pl.semaphore_signal(bar, inc=1, device_id=(peer(d), gz), device_id_type=MESH)

    loose = jnp.logical_not(in_span)
    cross_dn = has_dn & ((place == 0) | loose)
    cross_up = has_up & ((place == span - 1) | loose)
    n_bar = (
        (n_z - 1) + (n_zc - 1) + jnp.where(in_span, span - 1, 0)
        + cross_dn.astype(jnp.int32) + cross_up.astype(jnp.int32))

    @pl.when(cross_dn)
    def _():
        pl.semaphore_signal(bar, inc=1, device_id=(gy - 1, gz), device_id_type=MESH)

    @pl.when(cross_up)
    def _():
        pl.semaphore_signal(bar, inc=1, device_id=(gy + 1, gz), device_id_type=MESH)

    loads = []
    for c in range(3):
        loads.append(pltpu.make_async_copy(
            ve_hbm.at[c], vb.at[c, pl.ds(2, CY), pl.ds(8, CZ)], ld_sem.at[c]))
        loads.append(pltpu.make_async_copy(
            om_hbm.at[c], wb.at[c, pl.ds(2, CY), pl.ds(8, CZ)], ld_sem.at[3 + c]))
    for cp in loads:
        cp.start()

    ztile = jnp.zeros((8, NX), F32)

    def zfill(i, carry):
        for c in range(3):
            for buf in (vb, wb):
                buf[c, i + 2, pl.ds(0, 8), :] = ztile
                buf[c, i + 2, pl.ds(8 + CZ, 8), :] = ztile
            yb[c, i, pl.ds(0, 8), :] = ztile
            yb[c, i, pl.ds(8 + CZ, 8), :] = ztile
        return carry

    lax.fori_loop(0, CY, zfill, 0)

    def zero_y(lo):
        zrow = jnp.zeros((CZ, NX), F32)
        for c in range(3):
            for k in range(2):
                vb[c, lo + k, pl.ds(8, CZ), :] = zrow
                wb[c, lo + k, pl.ds(8, CZ), :] = zrow
                mb[c, lo + k] = zrow

    @pl.when(jnp.logical_not(has_dn))
    def _():
        zero_y(0)

    @pl.when(jnp.logical_not(has_up))
    def _():
        zero_y(CY + 2)

    vals[0:3, :] = cell_ref[...].astype(F32)
    vals[3:6, :] = frac_ref[...]
    my_block = gy * n_z + gz
    row8 = lax.broadcasted_iota(jnp.int32, (8, 128), 0)
    lane = lax.broadcasted_iota(jnp.int32, (8, 128), 1)
    ln128 = lax.broadcasted_iota(jnp.int32, (128, 128), 1)
    sb128 = lax.broadcasted_iota(jnp.int32, (128, 128), 0)
    base0 = pl.multiple_of(rb * 128, 128)
    base1 = pl.multiple_of(rb * 128 + 128, 128)
    o0 = jnp.broadcast_to(own_ref[pl.ds(base0, 128)].reshape(1, 128), (8, 128))
    o1 = jnp.broadcast_to(own_ref[pl.ds(base1, 128)].reshape(1, 128), (8, 128))
    own = jnp.where(row8 == 0, o0, jnp.where(row8 == 1, o1, -1))
    mine = own == my_block
    mf = mine.astype(F32)
    upper = (sb128 <= ln128).astype(F32)
    csum = jnp.dot(mf, upper, preferred_element_type=F32)
    tot0 = jnp.broadcast_to(csum[0:1, 127:128], (8, 128))
    rank = csum - mf + jnp.where(row8 == 1, tot0, 0.0)
    rank = jnp.where(mine, rank, -1.0)
    rank_t = jnp.transpose(jnp.concatenate([rank] * 16, axis=0))
    lanef = ln128.astype(F32)
    s0 = (jnp.broadcast_to(rank_t[:, 0:1], (128, 128)) == lanef).astype(F32)
    s1 = (jnp.broadcast_to(rank_t[:, 1:2], (128, 128)) == lanef).astype(F32)
    par = jnp.dot(vals[:, pl.ds(base0, 128)], s0, precision=HI, preferred_element_type=F32)
    par = par + jnp.dot(vals[:, pl.ds(base1, 128)], s1, precision=HI, preferred_element_type=F32)
    sel[0] = s0
    sel[1] = s1

    def table(n, k):
        rows = lax.broadcasted_iota(jnp.int32, (n, 128), 0).astype(F32)
        return m4((rows - par[k:k + 1, :]) - par[3 + k:4 + k, :])

    tx = table(NX, 0)
    tyq = table(CY, 1)
    tzq = table(CZ, 2)
    txs = split(tx)
    txb[0] = txs[0]
    txb[1] = txs[1]
    tzb[...] = tzq

    for cp in loads:
        cp.wait()

    def pack(i, carry):
        c = i // 4
        g = i % 4
        for f, buf in ((0, vb), (1, wb)):
            for j in range(4):
                y = 2 + 4 * g + j
                zs[0, f, c, g, 2 * j:2 * j + 2, :] = buf[c, y, 6 + CZ:8 + CZ, :]
                zs[1, f, c, g, 2 * j:2 * j + 2, :] = buf[c, y, 8:10, :]
        return carry

    lax.fori_loop(0, 12, pack, 0)

    def sample(y, acc):
        wyr = tyq_row(y)
        out = []
        for c in range(3):
            v = split(vb[c, y + 2, pl.ds(8, CZ), :])
            col = dot3(v, (txb[0], txb[1]), ((1,), (0,))) * tzb[...]
            s = jnp.sum(col, axis=0, keepdims=True)
            out.append(acc[c] + s * wyr)
        return tuple(out)

    ab[0] = tyq

    def tyq_row(y):
        return ab[0, pl.ds(y, 1), :]

    zrow1 = jnp.zeros((1, 128), F32)
    pvq = lax.fori_loop(0, CY, sample, (zrow1, zrow1, zrow1))
    qa = jnp.zeros((8, 128), F32)
    qb = qa
    for c in range(3):
        full = jnp.broadcast_to(pvq[c], (8, 128))
        qa = jnp.where(row8 == c, full, qa)
        qb = jnp.where(row8 == c + 4, full, qb)
    dnt = (((1,), (1,)), ((), ()))
    packet = lax.dot_general(qa, s0, dnt, precision=HI, preferred_element_type=F32)
    packet = packet + lax.dot_general(qb, s1, dnt, precision=HI, preferred_element_type=F32)

    def trig(rows, twist):
        col = lax.broadcasted_iota(jnp.int32, rows.shape, 1)
        station = col % BP
        blade = (2 * rows + col // BP) % BLADES
        theta = ang_ref[0].astype(F32) * turn_step
        theta = theta + 2.0 * 3.141592653589793 / 3.0 * blade.astype(F32)
        radius = (station.astype(F32) + 0.5) / BP
        return station, tip_speed * radius, jnp.cos(theta), jnp.sin(theta), jnp.cos(twist), jnp.sin(twist)

    def forces(angles, chord, pv):
        station, reach, cos_t, sin_t, cos_w, sin_w = angles
        rel_x = pv[0]
        rel_y = pv[1] + reach * sin_t
        rel_z = pv[2] - reach * cos_t
        rel_t = -sin_t * rel_y + cos_t * rel_z
        speed = jnp.sqrt(rel_x * rel_x + rel_t * rel_t + 1.0)
        gamma = 3.141592653589793 * chord * (rel_x * cos_w + rel_t * sin_w)
        before = jnp.where(station == 0, 0.0, pltpu.roll(gamma, 1, 1))
        ratio = (gamma - before) / speed
        return [ratio * rel_x, gamma * cos_t + ratio * rel_y, gamma * sin_t + ratio * rel_z]

    def pick(a, b):
        a, b = jnp.broadcast_to(a, (8, 128)), jnp.broadcast_to(b, (8, 128))
        return jnp.where(row8 == 0, a, jnp.where(row8 == 1, b, 0.0))

    def pair(ref):
        return pick(ref[pl.ds(base0, 128)].reshape(1, 128), ref[pl.ds(base1, 128)].reshape(1, 128))

    trig2 = trig(row8 + rb, pair(twist_ref))
    chord2 = pair(chord_ref)

    pl.semaphore_wait(bar, n_bar)

    def rcopy(src, dst, ss, rs, dev):
        return pltpu.make_async_remote_copy(
            src_ref=src, dst_ref=dst, send_sem=ss, recv_sem=rs, device_id=dev, device_id_type=MESH)

    def z_copy(d):
        return rcopy(zs.at[d], zr.at[d], zss.at[d], zsr.at[d], (gy, gz + (1 if d == 0 else -1)))

    PARTS = ((0, 8), (CZ - 8, 8), (8, CZ - 16))

    def y_copy(f, d, part):
        buf = vb if f == 0 else wb
        src, dst = (CY, 0) if d == 0 else (2, CY + 2)
        z0, n = PARTS[part]
        return rcopy(
            buf.at[:, pl.ds(src, 2), pl.ds(8 + z0, n)], buf.at[:, pl.ds(dst, 2), pl.ds(8 + z0, n)],
            ys.at[f, d, part], yr.at[f, d, part], (gy + (1 if d == 0 else -1), gz))

    def p1_copy(d):
        return rcopy(pk, p1r.at[gz - vb0], p1s.at[d - 1], p1v.at[gz - vb0],
                     (gy, lax.rem(gz + d, n_z)))

    @pl.when(is_src)
    def _():
        pk[...] = packet
        p1r[gz - vb0] = packet
        for d in range(1, n_z):
            p1_copy(d).start()

    up_cond = ((has_up, has_dn), (has_dn, has_up))
    rt_cond = ((has_r, has_l), (has_l, has_r))
    for d in range(2):
        @pl.when(rt_cond[d][0])
        def _():
            z_copy(d).start()

    for parts in ((0, 1), (2,)):
        for d in range(2):
            @pl.when(up_cond[d][0])
            def _():
                for f in range(2):
                    for part in parts:
                        y_copy(f, d, part).start()

    def wx_loop(y, carry):
        lanes = lax.broadcasted_iota(jnp.int32, (CHUNK, NX), 1)
        for z0 in range(0, CZ, CHUNK):
            w = remesh_weights(vb[0, y + 2, pl.ds(8 + z0, CHUNK), :])
            for k in range(5):
                s = k - 2
                x = w[k]
                if s > 0:
                    x = jnp.where(lanes < NX - s, x, 0.0)
                elif s < 0:
                    x = jnp.where(lanes >= -s, x, 0.0)
                wx[k, y, pl.ds(z0, CHUNK), :] = x
        return carry

    def wz_loop(y, carry):
        for z0 in range(0, CZ, CHUNK):
            w = remesh_weights(vb[2, y + 2, pl.ds(8 + z0, CHUNK), :])
            for k in range(5):
                wz[k, y, pl.ds(8 + z0, CHUNK), :] = w[k]
        return carry

    def wz_edge(y, carry):
        for r0 in (0, 8 + CZ):
            w = remesh_weights(vb[2, y + 2, pl.ds(r0, 8), :])
            for k in range(5):
                wz[k, y, pl.ds(r0, 8), :] = w[k]
        return carry

    def wy_one(y, rows):
        for z0, n in rows:
            w = remesh_weights(vb[1, y, pl.ds(8 + z0, n), :])
            for k in range(5):
                wy[k, y, pl.ds(z0, n), :] = w[k]

    def wy_loop(y, carry):
        wy_one(y + 2, ((0, CHUNK), (CHUNK, CHUNK)))
        return carry

    c0 = section_step / 12.0
    cl = section_step * viscosity / 12.0

    def around(buf, c, y, z0, n, dim):
        if dim == 2:
            return [buf[c, y + 2 + k, pl.ds(8 + z0, n), :] for k in (-2, -1, 1, 2)]
        if dim == 1:
            return [buf[c, y + 2, pl.ds(8 + z0 + k, n), :] for k in (-2, -1, 1, 2)]
        f = buf[c, y + 2, pl.ds(8 + z0, n), :]
        lanes = lax.broadcasted_iota(jnp.int32, (n, NX), 1)
        res = []
        for k in (-2, -1, 1, 2):
            r = pltpu.roll(f, (-k) % NX, 1)
            m = lanes >= -k if k < 0 else lanes < NX - k
            res.append(jnp.where(m, r, 0.0))
        return res

    def section_rows(y, rows):
        for z0, n in rows:
            om = [wb[c, y + 2, pl.ds(8 + z0, n), :] for c in range(3)]
            oms = [c0 * o for o in om]
            for c in range(3):
                acc = om[c]
                near = None
                far = None
                for dim in range(3):
                    a = around(vb, c, y, z0, n, dim)
                    acc = acc + oms[2 - dim] * (8.0 * (a[2] - a[1]) - (a[3] - a[0]))
                    b = around(wb, c, y, z0, n, dim)
                    p = b[1] + b[2]
                    e = b[0] + b[3]
                    near = p if near is None else near + p
                    far = e if far is None else far + e
                acc = acc + cl * (16.0 * near - far - 90.0 * om[c])
                sb[c, y, pl.ds(z0, n), :] = acc

    RIM = ((0, 8), (CZ - 8, 8))
    half = (CZ - 16) // 2
    MID = ((8, half), (8 + half, half))

    def edge_y(i):
        return jnp.where(i < 2, i, i + CY - 4)

    def run(n, fn):
        def step(i, carry):
            fn(i)
            return carry

        lax.fori_loop(0, n, step, 0)

    lax.fori_loop(0, CY, wx_loop, 0)
    run(CY - 4, lambda i: section_rows(i + 2, MID))

    def p1_wait(s):
        return rcopy(p1r.at[s], p1r.at[s], p1s.at[0], p1v.at[s], (gy, gz))

    def p2_copy(d):
        return rcopy(p2s, p2r.at[d], p2ss.at[d - 1], p2v.at[d], (peer(d), gz))

    @pl.when(in_span)
    def _():
        for s in range(nvb):
            @pl.when(gz != vb0 + s)
            def _():
                p1_wait(s).wait_recv()
        tile = p1r[0]
        for s in range(1, nvb):
            tile = tile + p1r[s]
        p2s[...] = tile
        p2r[0] = tile
        for d in range(1, span):
            p2_copy(d).start()

    lax.fori_loop(0, CY, wz_loop, 0)
    lax.fori_loop(0, CY, wy_loop, 0)

    for d in range(2):
        @pl.when(rt_cond[d][1])
        def _():
            z_copy(d).wait_recv()
            lo = 6 if d == 0 else 8 + CZ

            def unpack(i, carry):
                c = i // 4
                g = i % 4
                for f, buf in ((0, vb), (1, wb)):
                    for j in range(4):
                        buf[c, 2 + 4 * g + j, lo:lo + 2, :] = zr[d, f, c, g, 2 * j:2 * j + 2, :]
                return carry

            lax.fori_loop(0, 12, unpack, 0)

    lax.fori_loop(0, CY, wz_edge, 0)
    run(CY - 4, lambda i: section_rows(i + 2, RIM))

    for f in range(2):
        for d in range(2):
            @pl.when(up_cond[d][1])
            def _():
                for part in range(2):
                    y_copy(f, d, part).wait_recv()

    run(4, lambda i: section_rows(edge_y(i), RIM))
    for y in (0, 1, CY + 2, CY + 3):
        wy_one(y, RIM)

    def p3_copy(d):
        return rcopy(p3s, p3r.at[zc], p3ss.at[d - 1], p3v.at[zc],
                     (lax.rem(zc + d, n_zc) * 8 + plane, gz))

    @pl.when(in_span)
    def _():
        for d in range(1, span):
            rcopy(p2r.at[d], p2r.at[d], p2ss.at[0], p2v.at[d], (gy, gz)).wait_recv()
        tile = p2r[0]
        for d in range(1, span):
            tile = tile + p2r[d]
        p3s[...] = tile
        p3r[zc] = tile

    def smear_rows(y, spans):
        lhs = []
        for c in range(3):
            row = ab[c + 1, pl.ds(y, 1), :]
            for z0, n in spans:
                lhs.append(tzb[pl.ds(z0, n), :] * row)
        res = dot3(split(jnp.concatenate(lhs, axis=0)), (txb[0], txb[1]), ((1,), (1,)))
        at = 0
        for c in range(3):
            for z0, n in spans:
                sb[c, y, pl.ds(z0, n), :] = sb[c, y, pl.ds(z0, n), :] + res[at:at + n]
                at += n

    @pl.when(is_src)
    def _():
        tile = p3s[...]
        pv2 = [pick(tile[c:c + 1], tile[4 + c:5 + c]) for c in range(3)]
        src = forces(trig2, chord2, pv2)
        e0 = jnp.zeros((8, 128), F32)
        e1 = e0
        for c in range(3):
            e0 = jnp.where(row8 == c, jnp.broadcast_to(src[c][0:1], (8, 128)), e0)
            e1 = jnp.where(row8 == c, jnp.broadcast_to(src[c][1:2], (8, 128)), e1)
        srcq = jnp.dot(e0, sel[0], precision=HI, preferred_element_type=F32)
        srcq = srcq + jnp.dot(e1, sel[1], precision=HI, preferred_element_type=F32)
        for c in range(3):
            ab[c + 1] = section_step * ab[0] * srcq[c:c + 1, :]
        run(CY, lambda y: smear_rows(y, RIM))

    def move_x(y, rows):
        for z0, n in rows:
            for c in range(3):
                f = sb[c, y, pl.ds(z0, n), :]
                g = wx[2, y, pl.ds(z0, n), :] * f
                for k in (0, 1, 3, 4):
                    p = wx[k, y, pl.ds(z0, n), :] * f
                    g = g + pltpu.roll(p, (k - 2) % NX, 1)
                mb[c, y + 2, pl.ds(z0, n), :] = g

    def m_copy(d, part):
        src_y, dst_y = (CY, 0) if d == 0 else (2, CY + 2)
        z0, n = PARTS[part]
        return rcopy(mb.at[:, pl.ds(src_y, 2), pl.ds(z0, n)], mb.at[:, pl.ds(dst_y, 2), pl.ds(z0, n)],
                     ms.at[d, part], mr.at[d, part], (gy + (1 if d == 0 else -1), gz))

    run(4, lambda i: move_x(edge_y(i), RIM))
    for d in range(2):
        @pl.when(up_cond[d][0])
        def _():
            for part in range(2):
                m_copy(d, part).start()

    @pl.when(in_span)
    def _():
        for d in range(1, n_zc):
            p3_copy(d).start()

    for f in range(2):
        for d in range(2):
            @pl.when(up_cond[d][1])
            def _():
                y_copy(f, d, 2).wait_recv()

    run(4, lambda i: section_rows(edge_y(i), MID))

    @pl.when(is_src)
    def _():
        run(4, lambda i: smear_rows(edge_y(i), MID))

    run(4, lambda i: move_x(edge_y(i), MID))
    for d in range(2):
        @pl.when(up_cond[d][0])
        def _():
            m_copy(d, 2).start()

    run(CY - 4, lambda i: move_x(i + 2, RIM))

    def move_y(y, rows):
        for z0, n in rows:
            w = [wy[k, y + 4 - k, pl.ds(z0, n), :] for k in range(5)]
            for c in range(3):
                g = w[0] * mb[c, y + 4, pl.ds(z0, n), :]
                for k in range(1, 5):
                    g = g + w[k] * mb[c, y + 4 - k, pl.ds(z0, n), :]
                yb[c, y, pl.ds(8 + z0, n), :] = g

    run(CY - 4, lambda i: move_y(i + 2, RIM))
    for d in range(2):
        @pl.when(up_cond[d][1])
        def _():
            for part in range(2):
                m_copy(d, part).wait_recv()

    run(4, lambda i: move_y(edge_y(i), RIM))

    def pack2(i):
        c = i // 4
        g = i % 4
        for j in range(4):
            y = 4 * g + j
            ks[0, c, g, 2 * j:2 * j + 2, :] = yb[c, y, 6 + CZ:8 + CZ, :]
            ks[1, c, g, 2 * j:2 * j + 2, :] = yb[c, y, 8:10, :]

    run(12, pack2)

    def k_copy(d):
        return rcopy(ks.at[d], kr.at[d], kss.at[d], ksr.at[d], (gy, gz + (1 if d == 0 else -1)))

    for d in range(2):
        @pl.when(rt_cond[d][0])
        def _():
            k_copy(d).start()

    @pl.when(is_src)
    def _():
        run(CY - 4, lambda i: smear_rows(i + 2, MID))

    run(CY - 4, lambda i: move_x(i + 2, MID))
    for y in (0, 1, CY + 2, CY + 3):
        wy_one(y, MID)
    run(CY - 4, lambda i: move_y(i + 2, MID))
    for d in range(2):
        @pl.when(up_cond[d][1])
        def _():
            m_copy(d, 2).wait_recv()

    run(4, lambda i: move_y(edge_y(i), MID))

    def move_z(y, rows):
        for z0, n in rows:
            w = [wz[k, y, pl.ds(8 + z0 + 2 - k, n), :] for k in range(5)]
            for c in range(3):
                g = w[0] * yb[c, y, pl.ds(8 + z0 + 2, n), :]
                for k in range(1, 5):
                    g = g + w[k] * yb[c, y, pl.ds(8 + z0 + 2 - k, n), :]
                out_ref[c, y, pl.ds(z0, n), :] = g

    run(CY, lambda y: move_z(y, MID))

    for s in range(n_zc):
        @pl.when((zc != s) & (s * 8 + plane < NS))
        def _():
            rcopy(p3r.at[s], p3r.at[s], p3ss.at[0], p3v.at[s], (gy, gz)).wait_recv()

    for s in range(n_zc):
        @pl.when(s * 8 + plane < NS)
        def _():
            tall[(s * 8 + plane) // span] = p3r[s]

    for u in range(TURBINES // 2):
        e, o = tall[2 * u], tall[2 * u + 1]
        for c in range(3):
            pvb[c, 3 * u:3 * u + 1, :] = e[c:c + 1]
            pvb[c, 3 * u + 1:3 * u + 2, :] = e[4 + c:5 + c] + o[c:c + 1]
            pvb[c, 3 * u + 2:3 * u + 3, :] = o[4 + c:5 + c]
    n_rows = TURBINES * BLADES * BP // 128
    for r in range(n_rows):
        pvb[3, r:r + 1, :] = chord_ref[128 * r:128 * r + 128].reshape(1, 128)
        pvb[4, r:r + 1, :] = twist_ref[128 * r:128 * r + 128].reshape(1, 128)
    r16 = lax.broadcasted_iota(jnp.int32, (16, 128), 0)
    live = r16 < n_rows
    full = forces(
        trig(r16, jnp.where(live, pvb[4], 0.0)), jnp.where(live, pvb[3], 0.0),
        [jnp.where(live, pvb[c], 0.0) for c in range(3)])
    for r in range(n_rows):
        for c in range(3):
            src_out[c:c + 1, 128 * r:128 * r + 128] = full[c][r:r + 1]

    for d in range(2):
        @pl.when(rt_cond[d][1])
        def _():
            k_copy(d).wait_recv()
            lo = 6 if d == 0 else 8 + CZ

            def unpack2(i):
                c = i // 4
                g = i % 4
                for j in range(4):
                    yb[c, 4 * g + j, lo:lo + 2, :] = kr[d, c, g, 2 * j:2 * j + 2, :]

            run(12, unpack2)

    run(CY, lambda y: move_z(y, RIM))

    for d in range(2):
        @pl.when(rt_cond[d][0])
        def _():
            z_copy(d).wait_send()
            k_copy(d).wait_send()

        @pl.when(up_cond[d][0])
        def _():
            for part in range(3):
                y_copy(0, d, part).wait_send()
                y_copy(1, d, part).wait_send()
                m_copy(d, part).wait_send()

    @pl.when(is_src)
    def _():
        for d in range(1, n_z):
            p1_copy(d).wait_send()

    @pl.when(in_span)
    def _():
        for d in range(1, span):
            p2_copy(d).wait_send()
        for d in range(1, n_zc):
            p3_copy(d).wait_send()


def on_device(n_y, n_z, omega, velocity, owner, cells, frac, chord, twist, angle):
    _, cy, cz, nx = omega.shape
    n_p = owner.shape[0]
    n_zc = n_y // 8
    vm = pl.BlockSpec(memory_space=pltpu.VMEM)
    hb = pl.BlockSpec(memory_space=pl.ANY)
    sm = pl.BlockSpec(memory_space=pltpu.SMEM)
    nvb = max(n_z // 2, 1)
    V = pltpu.VMEM
    D = pltpu.SemaphoreType.DMA
    scratch = [
        V((3, cy + 4, cz + 16, nx), F32),
        V((3, cy + 4, cz + 16, nx), F32),
        V((3, cy, cz, nx), F32),
        V((3, cy + 4, cz, nx), F32),
        V((3, cy, cz + 16, nx), F32),
        V((5, cy, cz, nx), F32),
        V((5, cy + 4, cz, nx), F32),
        V((5, cy, cz + 16, nx), F32),
        V((2, 2, 3, cy // 4, 8, nx), F32),
        V((2, 2, 3, cy // 4, 8, nx), F32),
        V((2, 3, cy // 4, 8, nx), F32),
        V((2, 3, cy // 4, 8, nx), F32),
        V((8, n_p), F32),
        V((2, 128, 128), F32),
        V((8, 128), F32),
        V((nvb, 8, 128), F32),
        V((8, 128), F32),
        V((n_y // TURBINES, 8, 128), F32),
        V((8, 128), F32),
        V((n_zc, 8, 128), F32),
        V((5, 16, 128), F32),
        V((TURBINES, 8, 128), F32),
        V((4, cy, 128), F32),
        V((2, nx, 128), BF),
        V((cz, 128), F32),
        D((6,)), D((2, 2, 3)), D((2, 2, 3)), D((2,)), D((2,)),
        D((n_z - 1,)), D((nvb,)), D((n_y // TURBINES - 1,)), D((n_y // TURBINES,)), D((n_zc - 1,)), D((n_zc,)),
        D((2, 3)), D((2, 3)), D((2,)), D((2,)),
    ]
    out, src = pl.pallas_call(
        functools.partial(kernel, n_y, n_z),
        name="section",
        out_shape=(
            pltpu.VMEM(omega.shape, F32),
            jax.ShapeDtypeStruct((3, n_p), F32),
        ),
        in_specs=[hb, hb, vm, vm, vm, vm, vm, sm],
        out_specs=(vm, vm),
        scratch_shapes=scratch,
        compiler_params=pltpu.CompilerParams(
            collective_id=0, has_side_effects=True, vmem_limit_bytes=60 * 1024 * 1024),
    )(omega, velocity, owner, cells, frac, chord, twist, angle)
    return out, src


def solution(mesh):
    n_y, n_z = mesh.shape["gy"], mesh.shape["gz"]
    field = P(None, "gy", "gz", None)
    return jax.shard_map(
        functools.partial(on_device, n_y, n_z),
        mesh=mesh,
        in_specs=(field, field, P(), P(), P(), P(), P(), P()),
        out_specs=(field, P()),
        check_vma=False,
    )
```

```python
import functools

import jax
import jax.numpy as jnp
from jax import lax
from jax.experimental import pallas as pl
from jax.experimental.pallas import tpu as pltpu
from jax.sharding import PartitionSpec as P

TURBINES = 6
BLADES = 3
BP = 64
MESH = pl.DeviceIdType.MESH
HI = lax.Precision.HIGHEST

section_step = 0.4
viscosity = 0.05
tip_speed = 3.0
turn_step = 2.0 * 3.141592653589793 / 720.0
F32 = jnp.float32
BF = jnp.bfloat16

CHUNK = 32


def m4(shift):
    mag = jnp.abs(shift)
    inner = 1.0 + mag * mag * (1.5 * mag - 2.5)
    far = 2.0 - mag
    outer = 0.5 * far * far * (1.0 - mag)
    return jnp.where(mag < 1.0, inner, jnp.where(mag < 2.0, outer, 0.0))


def remesh_weights(v):
    a = jnp.minimum(section_step * jnp.abs(v), 1.0)
    b = 1.0 - a
    a2 = a * a
    b2 = b * b
    w0 = 1.0 + a2 * (1.5 * a - 2.5)
    w1 = 1.0 + b2 * (1.5 * b - 2.5)
    wm = -0.5 * a * b2
    w2 = -0.5 * a2 * b
    pos = v > 0.0
    return (
        jnp.where(pos, 0.0, w2),
        jnp.where(pos, wm, w1),
        w0,
        jnp.where(pos, w1, wm),
        jnp.where(pos, w2, 0.0),
    )


def split(x):
    hi = x.astype(BF)
    return hi, (x - hi.astype(F32)).astype(BF)


def dot3(a, b, dims):
    ah, al = a
    bh, bl = b
    dn = (dims, ((), ()))
    d = functools.partial(lax.dot_general, dimension_numbers=dn, preferred_element_type=F32)
    return d(ah, bh) + d(al, bh) + d(ah, bl)


def kernel(
    n_y, n_z,
    om_hbm, ve_hbm, own_h, cell_h, frac_h, chord_h, twist_h, ang_h,
    out_ref, src_out,
    vb, wb, sb, mb, yb, wx, wy, wz, zs, zr, ks, kr,
    vals, sel, pk, p1r, p2s, p2r, p3s, p3r, pvb, tall, ab, txb, tzb, own_ref, cell_ref, frac_ref, chord_ref, twist_ref, ang_ref,
    ld_sem, ys, yr, zss, zsr, p1s, p1v, p2ss, p2v, p3ss, p3v, ms, mr, kss, ksr,
):
    gy = lax.axis_index("gy")
    gz = lax.axis_index("gz")
    CY, CZ, NX = om_hbm.shape[1], om_hbm.shape[2], om_hbm.shape[3]
    span = n_y // TURBINES
    nvb = max(n_z // 2, 1)
    vb0 = (n_z - nvb) // 2
    NS = span * TURBINES
    zc = gy // 8
    plane = gy % 8
    t_own = jnp.minimum(gy // span, TURBINES - 1)
    rb = (3 * t_own) // 2
    n_zc = n_y // 8
    has_dn, has_up = gy > 0, gy < n_y - 1
    has_l, has_r = gz > 0, gz < n_z - 1
    in_span = gy < NS
    is_src = in_span & (gz >= vb0) & (gz < vb0 + nvb)
    place = gy % span

    def peer(d):
        return t_own * span + lax.rem(place + d, span)


    bar = pltpu.get_barrier_semaphore()
    for d in range(1, n_z):
        pl.semaphore_signal(bar, inc=1, device_id=(gy, lax.rem(gz + d, n_z)), device_id_type=MESH)
    for d in range(1, n_zc):
        pl.semaphore_signal(
            bar, inc=1, device_id=(lax.rem(zc + d, n_zc) * 8 + plane, gz), device_id_type=MESH)

    @pl.when(in_span)
    def _():
        for d in range(1, span):
            pl.semaphore_signal(bar, inc=1, device_id=(peer(d), gz), device_id_type=MESH)

    loose = jnp.logical_not(in_span)
    cross_dn = has_dn & ((place == 0) | loose)
    cross_up = has_up & ((place == span - 1) | loose)
    n_bar = (
        (n_z - 1) + (n_zc - 1) + jnp.where(in_span, span - 1, 0)
        + cross_dn.astype(jnp.int32) + cross_up.astype(jnp.int32))

    @pl.when(cross_dn)
    def _():
        pl.semaphore_signal(bar, inc=1, device_id=(gy - 1, gz), device_id_type=MESH)

    @pl.when(cross_up)
    def _():
        pl.semaphore_signal(bar, inc=1, device_id=(gy + 1, gz), device_id_type=MESH)

    loads = []
    small = []
    for i, (src, dst) in enumerate((
        (own_h, own_ref), (cell_h, cell_ref), (frac_h, frac_ref),
        (chord_h, chord_ref), (twist_h, twist_ref), (ang_h, ang_ref),
    )):
        small.append(pltpu.make_async_copy(src, dst, ld_sem.at[6 + i]))
    for cp in small:
        cp.start()
    for c in range(3):
        loads.append(pltpu.make_async_copy(
            ve_hbm.at[c], vb.at[c, pl.ds(2, CY), pl.ds(8, CZ)], ld_sem.at[c]))
        loads.append(pltpu.make_async_copy(
            om_hbm.at[c], wb.at[c, pl.ds(2, CY), pl.ds(8, CZ)], ld_sem.at[3 + c]))
    for cp in loads:
        cp.start()

    ztile = jnp.zeros((8, NX), F32)

    def zfill(i, carry):
        for c in range(3):
            for buf in (vb, wb):
                buf[c, i + 2, pl.ds(0, 8), :] = ztile
                buf[c, i + 2, pl.ds(8 + CZ, 8), :] = ztile
            yb[c, i, pl.ds(0, 8), :] = ztile
            yb[c, i, pl.ds(8 + CZ, 8), :] = ztile
        return carry

    lax.fori_loop(0, CY, zfill, 0)

    def zero_y(lo):
        zrow = jnp.zeros((CZ, NX), F32)
        for c in range(3):
            for k in range(2):
                vb[c, lo + k, pl.ds(8, CZ), :] = zrow
                wb[c, lo + k, pl.ds(8, CZ), :] = zrow
                mb[c, lo + k] = zrow

    @pl.when(jnp.logical_not(has_dn))
    def _():
        zero_y(0)

    @pl.when(jnp.logical_not(has_up))
    def _():
        zero_y(CY + 2)

    for cp in small:
        cp.wait()
    vals[0:3, :] = cell_ref[...].astype(F32)
    vals[3:6, :] = frac_ref[...]
    my_block = gy * n_z + gz
    row8 = lax.broadcasted_iota(jnp.int32, (8, 128), 0)
    lane = lax.broadcasted_iota(jnp.int32, (8, 128), 1)
    ln128 = lax.broadcasted_iota(jnp.int32, (128, 128), 1)
    sb128 = lax.broadcasted_iota(jnp.int32, (128, 128), 0)
    base0 = pl.multiple_of(rb * 128, 128)
    base1 = pl.multiple_of(rb * 128 + 128, 128)
    o0 = jnp.broadcast_to(own_ref[pl.ds(base0, 128)].reshape(1, 128), (8, 128))
    o1 = jnp.broadcast_to(own_ref[pl.ds(base1, 128)].reshape(1, 128), (8, 128))
    own = jnp.where(row8 == 0, o0, jnp.where(row8 == 1, o1, -1))
    mine = own == my_block
    mf = mine.astype(F32)
    upper = (sb128 <= ln128).astype(F32)
    csum = jnp.dot(mf, upper, preferred_element_type=F32)
    tot0 = jnp.broadcast_to(csum[0:1, 127:128], (8, 128))
    rank = csum - mf + jnp.where(row8 == 1, tot0, 0.0)
    rank = jnp.where(mine, rank, -1.0)
    rank_t = jnp.transpose(jnp.concatenate([rank] * 16, axis=0))
    lanef = ln128.astype(F32)
    s0 = (jnp.broadcast_to(rank_t[:, 0:1], (128, 128)) == lanef).astype(F32)
    s1 = (jnp.broadcast_to(rank_t[:, 1:2], (128, 128)) == lanef).astype(F32)
    par = jnp.dot(vals[:, pl.ds(base0, 128)], s0, precision=HI, preferred_element_type=F32)
    par = par + jnp.dot(vals[:, pl.ds(base1, 128)], s1, precision=HI, preferred_element_type=F32)
    sel[0] = s0
    sel[1] = s1

    def table(n, k):
        rows = lax.broadcasted_iota(jnp.int32, (n, 128), 0).astype(F32)
        return m4((rows - par[k:k + 1, :]) - par[3 + k:4 + k, :])

    tx = table(NX, 0)
    tyq = table(CY, 1)
    tzq = table(CZ, 2)
    txs = split(tx)
    txb[0] = txs[0]
    txb[1] = txs[1]
    tzb[...] = tzq

    for cp in loads:
        cp.wait()

    def pack(i, carry):
        c = i // 4
        g = i % 4
        for f, buf in ((0, vb), (1, wb)):
            for j in range(4):
                y = 2 + 4 * g + j
                zs[0, f, c, g, 2 * j:2 * j + 2, :] = buf[c, y, 6 + CZ:8 + CZ, :]
                zs[1, f, c, g, 2 * j:2 * j + 2, :] = buf[c, y, 8:10, :]
        return carry

    lax.fori_loop(0, 12, pack, 0)

    def sample(y, acc):
        wyr = tyq_row(y)
        out = []
        for c in range(3):
            v = split(vb[c, y + 2, pl.ds(8, CZ), :])
            col = dot3(v, (txb[0], txb[1]), ((1,), (0,))) * tzb[...]
            s = jnp.sum(col, axis=0, keepdims=True)
            out.append(acc[c] + s * wyr)
        return tuple(out)

    ab[0] = tyq

    def tyq_row(y):
        return ab[0, pl.ds(y, 1), :]

    zrow1 = jnp.zeros((1, 128), F32)
    pvq = lax.fori_loop(0, CY, sample, (zrow1, zrow1, zrow1))
    qa = jnp.zeros((8, 128), F32)
    qb = qa
    for c in range(3):
        full = jnp.broadcast_to(pvq[c], (8, 128))
        qa = jnp.where(row8 == c, full, qa)
        qb = jnp.where(row8 == c + 4, full, qb)
    dnt = (((1,), (1,)), ((), ()))
    packet = lax.dot_general(qa, s0, dnt, precision=HI, preferred_element_type=F32)
    packet = packet + lax.dot_general(qb, s1, dnt, precision=HI, preferred_element_type=F32)

    def trig(rows, twist):
        col = lax.broadcasted_iota(jnp.int32, rows.shape, 1)
        station = col % BP
        blade = (2 * rows + col // BP) % BLADES
        theta = ang_ref[0].astype(F32) * turn_step
        theta = theta + 2.0 * 3.141592653589793 / 3.0 * blade.astype(F32)
        radius = (station.astype(F32) + 0.5) / BP
        return station, tip_speed * radius, jnp.cos(theta), jnp.sin(theta), jnp.cos(twist), jnp.sin(twist)

    def forces(angles, chord, pv):
        station, reach, cos_t, sin_t, cos_w, sin_w = angles
        rel_x = pv[0]
        rel_y = pv[1] + reach * sin_t
        rel_z = pv[2] - reach * cos_t
        rel_t = -sin_t * rel_y + cos_t * rel_z
        speed = jnp.sqrt(rel_x * rel_x + rel_t * rel_t + 1.0)
        gamma = 3.141592653589793 * chord * (rel_x * cos_w + rel_t * sin_w)
        before = jnp.where(station == 0, 0.0, pltpu.roll(gamma, 1, 1))
        ratio = (gamma - before) / speed
        return [ratio * rel_x, gamma * cos_t + ratio * rel_y, gamma * sin_t + ratio * rel_z]

    def pick(a, b):
        a, b = jnp.broadcast_to(a, (8, 128)), jnp.broadcast_to(b, (8, 128))
        return jnp.where(row8 == 0, a, jnp.where(row8 == 1, b, 0.0))

    def pair(ref):
        return pick(ref[pl.ds(base0, 128)].reshape(1, 128), ref[pl.ds(base1, 128)].reshape(1, 128))

    trig2 = trig(row8 + rb, pair(twist_ref))
    chord2 = pair(chord_ref)

    pl.semaphore_wait(bar, n_bar)

    def rcopy(src, dst, ss, rs, dev):
        return pltpu.make_async_remote_copy(
            src_ref=src, dst_ref=dst, send_sem=ss, recv_sem=rs, device_id=dev, device_id_type=MESH)

    def z_copy(d):
        return rcopy(zs.at[d], zr.at[d], zss.at[d], zsr.at[d], (gy, gz + (1 if d == 0 else -1)))

    PARTS = ((0, 8), (CZ - 8, 8), (8, CZ - 16))

    def y_copy(f, d, part):
        buf = vb if f == 0 else wb
        src, dst = (CY, 0) if d == 0 else (2, CY + 2)
        z0, n = PARTS[part]
        return rcopy(
            buf.at[:, pl.ds(src, 2), pl.ds(8 + z0, n)], buf.at[:, pl.ds(dst, 2), pl.ds(8 + z0, n)],
            ys.at[f, d, part], yr.at[f, d, part], (gy + (1 if d == 0 else -1), gz))

    def p1_copy(d):
        return rcopy(pk, p1r.at[gz - vb0], p1s.at[d - 1], p1v.at[gz - vb0],
                     (gy, lax.rem(gz + d, n_z)))

    @pl.when(is_src)
    def _():
        pk[...] = packet
        p1r[gz - vb0] = packet
        for d in range(1, n_z):
            p1_copy(d).start()

    up_cond = ((has_up, has_dn), (has_dn, has_up))
    rt_cond = ((has_r, has_l), (has_l, has_r))
    for d in range(2):
        @pl.when(rt_cond[d][0])
        def _():
            z_copy(d).start()

    for d in range(2):
        @pl.when(up_cond[d][0])
        def _():
            for f in range(2):
                for part in range(2):
                    y_copy(f, d, part).start()

    def wx_loop(y, carry):
        lanes = lax.broadcasted_iota(jnp.int32, (CHUNK, NX), 1)
        for z0 in range(0, CZ, CHUNK):
            w = remesh_weights(vb[0, y + 2, pl.ds(8 + z0, CHUNK), :])
            for k in range(5):
                s = k - 2
                x = w[k]
                if s > 0:
                    x = jnp.where(lanes < NX - s, x, 0.0)
                elif s < 0:
                    x = jnp.where(lanes >= -s, x, 0.0)
                wx[k, y, pl.ds(z0, CHUNK), :] = x
        return carry

    def wz_loop(y, carry):
        for z0 in range(0, CZ, CHUNK):
            w = remesh_weights(vb[2, y + 2, pl.ds(8 + z0, CHUNK), :])
            for k in range(5):
                wz[k, y, pl.ds(8 + z0, CHUNK), :] = w[k]
        return carry

    def wz_edge(y, carry):
        for r0 in (0, 8 + CZ):
            w = remesh_weights(vb[2, y + 2, pl.ds(r0, 8), :])
            for k in range(5):
                wz[k, y, pl.ds(r0, 8), :] = w[k]
        return carry

    def wy_one(y, rows):
        for z0, n in rows:
            w = remesh_weights(vb[1, y, pl.ds(8 + z0, n), :])
            for k in range(5):
                wy[k, y, pl.ds(z0, n), :] = w[k]

    def wy_loop(y, carry):
        wy_one(y + 2, ((0, CHUNK), (CHUNK, CHUNK)))
        return carry

    c0 = section_step / 12.0
    cl = section_step * viscosity / 12.0

    def around(buf, c, y, z0, n, dim):
        if dim == 2:
            return [buf[c, y + 2 + k, pl.ds(8 + z0, n), :] for k in (-2, -1, 1, 2)]
        if dim == 1:
            return [buf[c, y + 2, pl.ds(8 + z0 + k, n), :] for k in (-2, -1, 1, 2)]
        f = buf[c, y + 2, pl.ds(8 + z0, n), :]
        lanes = lax.broadcasted_iota(jnp.int32, (n, NX), 1)
        res = []
        for k in (-2, -1, 1, 2):
            r = pltpu.roll(f, (-k) % NX, 1)
            m = lanes >= -k if k < 0 else lanes < NX - k
            res.append(jnp.where(m, r, 0.0))
        return res

    def section_rows(y, rows, dims=(0, 1, 2)):
        for z0, n in rows:
            om = [wb[c, y + 2, pl.ds(8 + z0, n), :] for c in range(3)]
            oms = {d: c0 * om[2 - d] for d in dims}
            for c in range(3):
                acc = om[c] if 0 in dims else sb[c, y, pl.ds(z0, n), :]
                near = None
                far = None
                for dim in dims:
                    a = around(vb, c, y, z0, n, dim)
                    acc = acc + oms[dim] * (8.0 * (a[2] - a[1]) - (a[3] - a[0]))
                    b = around(wb, c, y, z0, n, dim)
                    p = b[1] + b[2]
                    e = b[0] + b[3]
                    near = p if near is None else near + p
                    far = e if far is None else far + e
                acc = acc + cl * (16.0 * near - far - (30.0 * len(dims)) * om[c])
                sb[c, y, pl.ds(z0, n), :] = acc

    RIM = ((0, 8), (CZ - 8, 8))
    half = (CZ - 16) // 2
    MID = ((8, half), (8 + half, half))

    def edge_y(i):
        return jnp.where(i < 2, i, i + CY - 4)

    def run(n, fn):
        def step(i, carry):
            fn(i)
            return carry

        lax.fori_loop(0, n, step, 0)

    lax.fori_loop(0, CY, wx_loop, 0)
    run(CY - 4, lambda i: section_rows(i + 2, MID))
    run(4, lambda i: section_rows(edge_y(i), MID, (0, 1)))

    def p1_wait(s):
        return rcopy(p1r.at[s], p1r.at[s], p1s.at[0], p1v.at[s], (gy, gz))

    def p2_copy(d):
        return rcopy(p2s, p2r.at[d], p2ss.at[d - 1], p2v.at[d], (peer(d), gz))

    @pl.when(in_span)
    def _():
        for s in range(nvb):
            @pl.when(gz != vb0 + s)
            def _():
                p1_wait(s).wait_recv()
        tile = p1r[0]
        for s in range(1, nvb):
            tile = tile + p1r[s]
        p2s[...] = tile
        p2r[0] = tile
        for d in range(1, span):
            p2_copy(d).start()

    for d in range(2):
        @pl.when(up_cond[d][0])
        def _():
            y_copy(0, d, 2).start()
            y_copy(1, d, 2).start()

    lax.fori_loop(0, CY, wz_loop, 0)
    lax.fori_loop(0, CY, wy_loop, 0)

    for d in range(2):
        @pl.when(rt_cond[d][1])
        def _():
            z_copy(d).wait_recv()
            lo = 6 if d == 0 else 8 + CZ

            def unpack(i, carry):
                c = i // 4
                g = i % 4
                for f, buf in ((0, vb), (1, wb)):
                    for j in range(4):
                        buf[c, 2 + 4 * g + j, lo:lo + 2, :] = zr[d, f, c, g, 2 * j:2 * j + 2, :]
                return carry

            lax.fori_loop(0, 12, unpack, 0)

    lax.fori_loop(0, CY, wz_edge, 0)
    run(4, lambda i: section_rows(edge_y(i), RIM, (0, 1)))
    run(CY - 4, lambda i: section_rows(i + 2, RIM))

    for f in range(2):
        for d in range(2):
            @pl.when(up_cond[d][1])
            def _():
                for part in range(2):
                    y_copy(f, d, part).wait_recv()

    run(4, lambda i: section_rows(edge_y(i), RIM, (2,)))
    for y in (0, 1, CY + 2, CY + 3):
        wy_one(y, RIM)

    def p3_copy(d):
        return rcopy(p3s, p3r.at[zc], p3ss.at[d - 1], p3v.at[zc],
                     (lax.rem(zc + d, n_zc) * 8 + plane, gz))

    @pl.when(in_span)
    def _():
        for d in range(1, span):
            rcopy(p2r.at[d], p2r.at[d], p2ss.at[0], p2v.at[d], (gy, gz)).wait_recv()
        tile = p2r[0]
        for d in range(1, span):
            tile = tile + p2r[d]
        p3s[...] = tile
        p3r[zc] = tile

    def smear_rows(y, spans):
        lhs = []
        for c in range(3):
            row = ab[c + 1, pl.ds(y, 1), :]
            for z0, n in spans:
                lhs.append(tzb[pl.ds(z0, n), :] * row)
        res = dot3(split(jnp.concatenate(lhs, axis=0)), (txb[0], txb[1]), ((1,), (1,)))
        at = 0
        for c in range(3):
            for z0, n in spans:
                sb[c, y, pl.ds(z0, n), :] = sb[c, y, pl.ds(z0, n), :] + res[at:at + n]
                at += n

    @pl.when(is_src)
    def _():
        tile = p3s[...]
        pv2 = [pick(tile[c:c + 1], tile[4 + c:5 + c]) for c in range(3)]
        src = forces(trig2, chord2, pv2)
        e0 = jnp.zeros((8, 128), F32)
        e1 = e0
        for c in range(3):
            e0 = jnp.where(row8 == c, jnp.broadcast_to(src[c][0:1], (8, 128)), e0)
            e1 = jnp.where(row8 == c, jnp.broadcast_to(src[c][1:2], (8, 128)), e1)
        srcq = jnp.dot(e0, sel[0], precision=HI, preferred_element_type=F32)
        srcq = srcq + jnp.dot(e1, sel[1], precision=HI, preferred_element_type=F32)
        for c in range(3):
            ab[c + 1] = section_step * ab[0] * srcq[c:c + 1, :]
        run(4, lambda i: smear_rows(edge_y(i), RIM))

    def move_x(y, rows):
        for z0, n in rows:
            for c in range(3):
                f = sb[c, y, pl.ds(z0, n), :]
                g = wx[2, y, pl.ds(z0, n), :] * f
                for k in (0, 1, 3, 4):
                    p = wx[k, y, pl.ds(z0, n), :] * f
                    g = g + pltpu.roll(p, (k - 2) % NX, 1)
                mb[c, y + 2, pl.ds(z0, n), :] = g

    def m_copy(d, part):
        src_y, dst_y = (CY, 0) if d == 0 else (2, CY + 2)
        z0, n = PARTS[part]
        return rcopy(mb.at[:, pl.ds(src_y, 2), pl.ds(z0, n)], mb.at[:, pl.ds(dst_y, 2), pl.ds(z0, n)],
                     ms.at[d, part], mr.at[d, part], (gy + (1 if d == 0 else -1), gz))

    run(4, lambda i: move_x(edge_y(i), RIM))
    for d in range(2):
        @pl.when(up_cond[d][0])
        def _():
            for part in range(2):
                m_copy(d, part).start()

    @pl.when(in_span)
    def _():
        for d in range(1, n_zc):
            p3_copy(d).start()

    @pl.when(is_src)
    def _():
        run(CY - 4, lambda i: smear_rows(i + 2, RIM))

    for f in range(2):
        for d in range(2):
            @pl.when(up_cond[d][1])
            def _():
                y_copy(f, d, 2).wait_recv()

    run(4, lambda i: section_rows(edge_y(i), MID, (2,)))

    @pl.when(is_src)
    def _():
        run(4, lambda i: smear_rows(edge_y(i), MID))

    run(4, lambda i: move_x(edge_y(i), MID))
    for d in range(2):
        @pl.when(up_cond[d][0])
        def _():
            m_copy(d, 2).start()

    run(CY - 4, lambda i: move_x(i + 2, RIM))

    def move_y(y, rows):
        for z0, n in rows:
            w = [wy[k, y + 4 - k, pl.ds(z0, n), :] for k in range(5)]
            for c in range(3):
                g = w[0] * mb[c, y + 4, pl.ds(z0, n), :]
                for k in range(1, 5):
                    g = g + w[k] * mb[c, y + 4 - k, pl.ds(z0, n), :]
                yb[c, y, pl.ds(8 + z0, n), :] = g

    run(CY - 4, lambda i: move_y(i + 2, RIM))
    for d in range(2):
        @pl.when(up_cond[d][1])
        def _():
            for part in range(2):
                m_copy(d, part).wait_recv()

    run(4, lambda i: move_y(edge_y(i), RIM))

    def pack2(i):
        c = i // 4
        g = i % 4
        for j in range(4):
            y = 4 * g + j
            ks[0, c, g, 2 * j:2 * j + 2, :] = yb[c, y, 6 + CZ:8 + CZ, :]
            ks[1, c, g, 2 * j:2 * j + 2, :] = yb[c, y, 8:10, :]

    run(12, pack2)

    def k_copy(d):
        return rcopy(ks.at[d], kr.at[d], kss.at[d], ksr.at[d], (gy, gz + (1 if d == 0 else -1)))

    for d in range(2):
        @pl.when(rt_cond[d][0])
        def _():
            k_copy(d).start()

    @pl.when(is_src)
    def _():
        run(CY - 4, lambda i: smear_rows(i + 2, MID))

    run(CY - 4, lambda i: move_x(i + 2, MID))
    for y in (0, 1, CY + 2, CY + 3):
        wy_one(y, MID)
    run(CY - 4, lambda i: move_y(i + 2, MID))
    for d in range(2):
        @pl.when(up_cond[d][1])
        def _():
            m_copy(d, 2).wait_recv()

    run(4, lambda i: move_y(edge_y(i), MID))

    def move_z(y, rows):
        for z0, n in rows:
            w = [wz[k, y, pl.ds(8 + z0 + 2 - k, n), :] for k in range(5)]
            for c in range(3):
                g = w[0] * yb[c, y, pl.ds(8 + z0 + 2, n), :]
                for k in range(1, 5):
                    g = g + w[k] * yb[c, y, pl.ds(8 + z0 + 2 - k, n), :]
                out_ref[c, y, pl.ds(z0, n), :] = g

    run(CY, lambda y: move_z(y, MID))

    for s in range(n_zc):
        @pl.when((zc != s) & (s * 8 + plane < NS))
        def _():
            rcopy(p3r.at[s], p3r.at[s], p3ss.at[0], p3v.at[s], (gy, gz)).wait_recv()

    for s in range(n_zc):
        @pl.when(s * 8 + plane < NS)
        def _():
            tall[(s * 8 + plane) // span] = p3r[s]

    for u in range(TURBINES // 2):
        e, o = tall[2 * u], tall[2 * u + 1]
        for c in range(3):
            pvb[c, 3 * u:3 * u + 1, :] = e[c:c + 1]
            pvb[c, 3 * u + 1:3 * u + 2, :] = e[4 + c:5 + c] + o[c:c + 1]
            pvb[c, 3 * u + 2:3 * u + 3, :] = o[4 + c:5 + c]
    n_rows = TURBINES * BLADES * BP // 128
    for r in range(n_rows):
        pvb[3, r:r + 1, :] = chord_ref[128 * r:128 * r + 128].reshape(1, 128)
        pvb[4, r:r + 1, :] = twist_ref[128 * r:128 * r + 128].reshape(1, 128)
    r16 = lax.broadcasted_iota(jnp.int32, (16, 128), 0)
    live = r16 < n_rows
    full = forces(
        trig(r16, jnp.where(live, pvb[4], 0.0)), jnp.where(live, pvb[3], 0.0),
        [jnp.where(live, pvb[c], 0.0) for c in range(3)])
    for r in range(n_rows):
        for c in range(3):
            src_out[c:c + 1, 128 * r:128 * r + 128] = full[c][r:r + 1]

    for d in range(2):
        @pl.when(rt_cond[d][1])
        def _():
            k_copy(d).wait_recv()
            lo = 6 if d == 0 else 8 + CZ

            def unpack2(i):
                c = i // 4
                g = i % 4
                for j in range(4):
                    yb[c, 4 * g + j, lo:lo + 2, :] = kr[d, c, g, 2 * j:2 * j + 2, :]

            run(12, unpack2)

    run(CY, lambda y: move_z(y, RIM))

    for d in range(2):
        @pl.when(rt_cond[d][0])
        def _():
            z_copy(d).wait_send()
            k_copy(d).wait_send()

        @pl.when(up_cond[d][0])
        def _():
            for part in range(3):
                y_copy(0, d, part).wait_send()
                y_copy(1, d, part).wait_send()
                m_copy(d, part).wait_send()

    @pl.when(is_src)
    def _():
        for d in range(1, n_z):
            p1_copy(d).wait_send()

    @pl.when(in_span)
    def _():
        for d in range(1, span):
            p2_copy(d).wait_send()
        for d in range(1, n_zc):
            p3_copy(d).wait_send()


def on_device(n_y, n_z, omega, velocity, owner, cells, frac, chord, twist, angle):
    _, cy, cz, nx = omega.shape
    n_p = owner.shape[0]
    n_zc = n_y // 8
    vm = pl.BlockSpec(memory_space=pltpu.VMEM)
    hb = pl.BlockSpec(memory_space=pl.ANY)
    nvb = max(n_z // 2, 1)
    V = pltpu.VMEM
    D = pltpu.SemaphoreType.DMA
    scratch = [
        V((3, cy + 4, cz + 16, nx), F32),
        V((3, cy + 4, cz + 16, nx), F32),
        V((3, cy, cz, nx), F32),
        V((3, cy + 4, cz, nx), F32),
        V((3, cy, cz + 16, nx), F32),
        V((5, cy, cz, nx), F32),
        V((5, cy + 4, cz, nx), F32),
        V((5, cy, cz + 16, nx), F32),
        V((2, 2, 3, cy // 4, 8, nx), F32),
        V((2, 2, 3, cy // 4, 8, nx), F32),
        V((2, 3, cy // 4, 8, nx), F32),
        V((2, 3, cy // 4, 8, nx), F32),
        V((8, n_p), F32),
        V((2, 128, 128), F32),
        V((8, 128), F32),
        V((nvb, 8, 128), F32),
        V((8, 128), F32),
        V((n_y // TURBINES, 8, 128), F32),
        V((8, 128), F32),
        V((n_zc, 8, 128), F32),
        V((5, 16, 128), F32),
        V((TURBINES, 8, 128), F32),
        V((4, cy, 128), F32),
        V((2, nx, 128), BF),
        V((cz, 128), F32),
        V((n_p,), jnp.int32), V((3, n_p), jnp.int32), V((3, n_p), F32), V((n_p,), F32), V((n_p,), F32),
        pltpu.SMEM((1,), jnp.int32),
        D((12,)), D((2, 2, 3)), D((2, 2, 3)), D((2,)), D((2,)),
        D((n_z - 1,)), D((nvb,)), D((n_y // TURBINES - 1,)), D((n_y // TURBINES,)), D((n_zc - 1,)), D((n_zc,)),
        D((2, 3)), D((2, 3)), D((2,)), D((2,)),
    ]
    out, src = pl.pallas_call(
        functools.partial(kernel, n_y, n_z),
        name="section",
        out_shape=(
            pltpu.VMEM(omega.shape, F32),
            V((3, n_p), F32),
        ),
        in_specs=[hb] * 8,
        out_specs=(vm, vm),
        scratch_shapes=scratch,
        compiler_params=pltpu.CompilerParams(
            collective_id=0, has_side_effects=True, vmem_limit_bytes=60 * 1024 * 1024),
    )(omega, velocity, owner, cells, frac, chord, twist, angle)
    return out, src


def solution(mesh):
    n_y, n_z = mesh.shape["gy"], mesh.shape["gz"]
    field = P(None, "gy", "gz", None)
    return jax.shard_map(
        functools.partial(on_device, n_y, n_z),
        mesh=mesh,
        in_specs=(field, field, P(), P(), P(), P(), P(), P()),
        out_specs=(field, P()),
        check_vma=False,
    )
```

```python
import functools

import jax
import jax.numpy as jnp
from jax import lax
from jax.experimental import pallas as pl
from jax.experimental.pallas import tpu as pltpu
from jax.sharding import PartitionSpec as P

TURBINES = 6
BLADES = 3
BP = 64
MESH = pl.DeviceIdType.MESH
HI = lax.Precision.HIGHEST

section_step = 0.4
viscosity = 0.05
tip_speed = 3.0
turn_step = 2.0 * 3.141592653589793 / 720.0
F32 = jnp.float32
BF = jnp.bfloat16

CHUNK = 32


def m4(shift):
    mag = jnp.abs(shift)
    inner = 1.0 + mag * mag * (1.5 * mag - 2.5)
    far = 2.0 - mag
    outer = 0.5 * far * far * (1.0 - mag)
    return jnp.where(mag < 1.0, inner, jnp.where(mag < 2.0, outer, 0.0))


def remesh_weights(v):
    a = jnp.minimum(section_step * jnp.abs(v), 1.0)
    b = 1.0 - a
    a2 = a * a
    b2 = b * b
    w0 = 1.0 + a2 * (1.5 * a - 2.5)
    w1 = 1.0 + b2 * (1.5 * b - 2.5)
    wm = -0.5 * a * b2
    w2 = -0.5 * a2 * b
    pos = v > 0.0
    return (
        jnp.where(pos, 0.0, w2),
        jnp.where(pos, wm, w1),
        w0,
        jnp.where(pos, w1, wm),
        jnp.where(pos, w2, 0.0),
    )


def split(x):
    hi = x.astype(BF)
    return hi, (x - hi.astype(F32)).astype(BF)


def dot3(a, b, dims):
    ah, al = a
    bh, bl = b
    dn = (dims, ((), ()))
    d = functools.partial(lax.dot_general, dimension_numbers=dn, preferred_element_type=F32)
    return d(ah, bh) + d(al, bh) + d(ah, bl)


def kernel(
    n_y, n_z,
    om_hbm, ve_hbm, own_h, cell_h, frac_h, chord_h, twist_h, ang_h,
    out_ref, src_out,
    vb, wb, sb, mb, yb, wx, wy, wz, zs, zr, ks, kr,
    vals, sel, pk, p1r, p2s, p2r, p3s, p3r, pvb, tall, ab, txb, tzb, own_ref, cell_ref, frac_ref, chord_ref, twist_ref, ang_ref,
    ld_sem, ys, yr, zss, zsr, p1s, p1v, p2ss, p2v, p3ss, p3v, ms, mr, kss, ksr,
):
    gy = lax.axis_index("gy")
    gz = lax.axis_index("gz")
    CY, CZ, NX = om_hbm.shape[1], om_hbm.shape[2], om_hbm.shape[3]
    span = n_y // TURBINES
    nvb = max(n_z // 2, 1)
    vb0 = (n_z - nvb) // 2
    NS = span * TURBINES
    zc = gy // 8
    plane = gy % 8
    t_own = jnp.minimum(gy // span, TURBINES - 1)
    rb = (3 * t_own) // 2
    n_zc = n_y // 8
    has_dn, has_up = gy > 0, gy < n_y - 1
    has_l, has_r = gz > 0, gz < n_z - 1
    in_span = gy < NS
    is_src = in_span & (gz >= vb0) & (gz < vb0 + nvb)
    place = gy % span

    def peer(d):
        return t_own * span + lax.rem(place + d, span)


    bar = pltpu.get_barrier_semaphore()
    for d in range(1, n_z):
        pl.semaphore_signal(bar, inc=1, device_id=(gy, lax.rem(gz + d, n_z)), device_id_type=MESH)
    for d in range(1, n_zc):
        pl.semaphore_signal(
            bar, inc=1, device_id=(lax.rem(zc + d, n_zc) * 8 + plane, gz), device_id_type=MESH)

    @pl.when(in_span)
    def _():
        for d in range(1, span):
            pl.semaphore_signal(bar, inc=1, device_id=(peer(d), gz), device_id_type=MESH)

    loose = jnp.logical_not(in_span)
    cross_dn = has_dn & ((place == 0) | loose)
    cross_up = has_up & ((place == span - 1) | loose)
    n_bar = (
        (n_z - 1) + (n_zc - 1) + jnp.where(in_span, span - 1, 0)
        + cross_dn.astype(jnp.int32) + cross_up.astype(jnp.int32))

    @pl.when(cross_dn)
    def _():
        pl.semaphore_signal(bar, inc=1, device_id=(gy - 1, gz), device_id_type=MESH)

    @pl.when(cross_up)
    def _():
        pl.semaphore_signal(bar, inc=1, device_id=(gy + 1, gz), device_id_type=MESH)

    loads = []
    small = []
    for i, (src, dst) in enumerate((
        (own_h, own_ref), (cell_h, cell_ref), (frac_h, frac_ref),
        (chord_h, chord_ref), (twist_h, twist_ref), (ang_h, ang_ref),
    )):
        small.append(pltpu.make_async_copy(src, dst, ld_sem.at[6 + i]))
    for cp in small:
        cp.start()
    for c in range(3):
        loads.append(pltpu.make_async_copy(
            ve_hbm.at[c], vb.at[c, pl.ds(2, CY), pl.ds(8, CZ)], ld_sem.at[c]))
        loads.append(pltpu.make_async_copy(
            om_hbm.at[c], wb.at[c, pl.ds(2, CY), pl.ds(8, CZ)], ld_sem.at[3 + c]))
    for cp in loads:
        cp.start()

    ztile = jnp.zeros((8, NX), F32)

    def zfill(i, carry):
        for c in range(3):
            for buf in (vb, wb):
                buf[c, i + 2, pl.ds(0, 8), :] = ztile
                buf[c, i + 2, pl.ds(8 + CZ, 8), :] = ztile
            yb[c, i, pl.ds(0, 8), :] = ztile
            yb[c, i, pl.ds(8 + CZ, 8), :] = ztile
        return carry

    lax.fori_loop(0, CY, zfill, 0)

    def zero_y(lo):
        zrow = jnp.zeros((CZ, NX), F32)
        for c in range(3):
            for k in range(2):
                vb[c, lo + k, pl.ds(8, CZ), :] = zrow
                wb[c, lo + k, pl.ds(8, CZ), :] = zrow
                mb[c, lo + k] = zrow

    @pl.when(jnp.logical_not(has_dn))
    def _():
        zero_y(0)

    @pl.when(jnp.logical_not(has_up))
    def _():
        zero_y(CY + 2)

    for cp in small:
        cp.wait()
    vals[0:3, :] = cell_ref[...].astype(F32)
    vals[3:6, :] = frac_ref[...]
    my_block = gy * n_z + gz
    row8 = lax.broadcasted_iota(jnp.int32, (8, 128), 0)
    lane = lax.broadcasted_iota(jnp.int32, (8, 128), 1)
    ln128 = lax.broadcasted_iota(jnp.int32, (128, 128), 1)
    sb128 = lax.broadcasted_iota(jnp.int32, (128, 128), 0)
    base0 = pl.multiple_of(rb * 128, 128)
    base1 = pl.multiple_of(rb * 128 + 128, 128)
    o0 = jnp.broadcast_to(own_ref[pl.ds(base0, 128)].reshape(1, 128), (8, 128))
    o1 = jnp.broadcast_to(own_ref[pl.ds(base1, 128)].reshape(1, 128), (8, 128))
    own = jnp.where(row8 == 0, o0, jnp.where(row8 == 1, o1, -1))
    mine = own == my_block
    mf = mine.astype(F32)
    upper = (sb128 <= ln128).astype(F32)
    csum = jnp.dot(mf, upper, preferred_element_type=F32)
    tot0 = jnp.broadcast_to(csum[0:1, 127:128], (8, 128))
    rank = csum - mf + jnp.where(row8 == 1, tot0, 0.0)
    rank = jnp.where(mine, rank, -1.0)
    rank_t = jnp.transpose(jnp.concatenate([rank] * 16, axis=0))
    lanef = ln128.astype(F32)
    s0 = (jnp.broadcast_to(rank_t[:, 0:1], (128, 128)) == lanef).astype(F32)
    s1 = (jnp.broadcast_to(rank_t[:, 1:2], (128, 128)) == lanef).astype(F32)
    par = jnp.dot(vals[:, pl.ds(base0, 128)], s0, precision=HI, preferred_element_type=F32)
    par = par + jnp.dot(vals[:, pl.ds(base1, 128)], s1, precision=HI, preferred_element_type=F32)
    sel[0] = s0
    sel[1] = s1

    def table(n, k):
        rows = lax.broadcasted_iota(jnp.int32, (n, 128), 0).astype(F32)
        return m4((rows - par[k:k + 1, :]) - par[3 + k:4 + k, :])

    tx = table(NX, 0)
    tyq = table(CY, 1)
    tzq = table(CZ, 2)
    txs = split(tx)
    txb[0] = txs[0]
    txb[1] = txs[1]
    tzb[...] = tzq

    for cp in loads:
        cp.wait()

    def pack(i, carry):
        c = i // 4
        g = i % 4
        for f, buf in ((0, vb), (1, wb)):
            for j in range(4):
                y = 2 + 4 * g + j
                zs[0, f, c, g, 2 * j:2 * j + 2, :] = buf[c, y, 6 + CZ:8 + CZ, :]
                zs[1, f, c, g, 2 * j:2 * j + 2, :] = buf[c, y, 8:10, :]
        return carry

    lax.fori_loop(0, 12, pack, 0)

    def sample(y, acc):
        wyr = tyq_row(y)
        out = []
        for c in range(3):
            v = split(vb[c, y + 2, pl.ds(8, CZ), :])
            col = dot3(v, (txb[0], txb[1]), ((1,), (0,))) * tzb[...]
            s = jnp.sum(col, axis=0, keepdims=True)
            out.append(acc[c] + s * wyr)
        return tuple(out)

    ab[0] = tyq

    def tyq_row(y):
        return ab[0, pl.ds(y, 1), :]

    zrow1 = jnp.zeros((1, 128), F32)
    pvq = lax.fori_loop(0, CY, sample, (zrow1, zrow1, zrow1))
    qa = jnp.zeros((8, 128), F32)
    qb = qa
    for c in range(3):
        full = jnp.broadcast_to(pvq[c], (8, 128))
        qa = jnp.where(row8 == c, full, qa)
        qb = jnp.where(row8 == c + 4, full, qb)
    dnt = (((1,), (1,)), ((), ()))
    packet = lax.dot_general(qa, s0, dnt, precision=HI, preferred_element_type=F32)
    packet = packet + lax.dot_general(qb, s1, dnt, precision=HI, preferred_element_type=F32)

    def trig(rows, twist):
        col = lax.broadcasted_iota(jnp.int32, rows.shape, 1)
        station = col % BP
        blade = (2 * rows + col // BP) % BLADES
        theta = ang_ref[0].astype(F32) * turn_step
        theta = theta + 2.0 * 3.141592653589793 / 3.0 * blade.astype(F32)
        radius = (station.astype(F32) + 0.5) / BP
        return station, tip_speed * radius, jnp.cos(theta), jnp.sin(theta), jnp.cos(twist), jnp.sin(twist)

    def forces(angles, chord, pv):
        station, reach, cos_t, sin_t, cos_w, sin_w = angles
        rel_x = pv[0]
        rel_y = pv[1] + reach * sin_t
        rel_z = pv[2] - reach * cos_t
        rel_t = -sin_t * rel_y + cos_t * rel_z
        speed = jnp.sqrt(rel_x * rel_x + rel_t * rel_t + 1.0)
        gamma = 3.141592653589793 * chord * (rel_x * cos_w + rel_t * sin_w)
        before = jnp.where(station == 0, 0.0, pltpu.roll(gamma, 1, 1))
        ratio = (gamma - before) / speed
        return [ratio * rel_x, gamma * cos_t + ratio * rel_y, gamma * sin_t + ratio * rel_z]

    def pick(a, b):
        a, b = jnp.broadcast_to(a, (8, 128)), jnp.broadcast_to(b, (8, 128))
        return jnp.where(row8 == 0, a, jnp.where(row8 == 1, b, 0.0))

    def pair(ref):
        return pick(ref[pl.ds(base0, 128)].reshape(1, 128), ref[pl.ds(base1, 128)].reshape(1, 128))

    trig2 = trig(row8 + rb, pair(twist_ref))
    chord2 = pair(chord_ref)

    pl.semaphore_wait(bar, n_bar)

    def rcopy(src, dst, ss, rs, dev):
        return pltpu.make_async_remote_copy(
            src_ref=src, dst_ref=dst, send_sem=ss, recv_sem=rs, device_id=dev, device_id_type=MESH)

    def z_copy(d):
        return rcopy(zs.at[d], zr.at[d], zss.at[d], zsr.at[d], (gy, gz + (1 if d == 0 else -1)))

    PARTS = ((0, 8), (CZ - 8, 8), (8, CZ - 16))

    def y_copy(f, d, part):
        buf = vb if f == 0 else wb
        src, dst = (CY, 0) if d == 0 else (2, CY + 2)
        z0, n = PARTS[part]
        return rcopy(
            buf.at[:, pl.ds(src, 2), pl.ds(8 + z0, n)], buf.at[:, pl.ds(dst, 2), pl.ds(8 + z0, n)],
            ys.at[f, d, part], yr.at[f, d, part], (gy + (1 if d == 0 else -1), gz))

    def p1_copy(d):
        return rcopy(pk, p1r.at[gz - vb0], p1s.at[d - 1], p1v.at[gz - vb0],
                     (gy, lax.rem(gz + d, n_z)))

    @pl.when(is_src)
    def _():
        pk[...] = packet
        p1r[gz - vb0] = packet
        for d in range(1, n_z):
            p1_copy(d).start()

    up_cond = ((has_up, has_dn), (has_dn, has_up))
    rt_cond = ((has_r, has_l), (has_l, has_r))
    for d in range(2):
        @pl.when(rt_cond[d][0])
        def _():
            z_copy(d).start()

    for d in range(2):
        @pl.when(up_cond[d][0])
        def _():
            for f in range(2):
                for part in range(2):
                    y_copy(f, d, part).start()

    def wx_loop(y, carry):
        lanes = lax.broadcasted_iota(jnp.int32, (CHUNK, NX), 1)
        for z0 in range(0, CZ, CHUNK):
            w = remesh_weights(vb[0, y + 2, pl.ds(8 + z0, CHUNK), :])
            for k in range(5):
                s = k - 2
                x = w[k]
                if s > 0:
                    x = jnp.where(lanes < NX - s, x, 0.0)
                elif s < 0:
                    x = jnp.where(lanes >= -s, x, 0.0)
                wx[k, y, pl.ds(z0, CHUNK), :] = x
        return carry

    def wz_loop(y, carry):
        for z0 in range(0, CZ, CHUNK):
            w = remesh_weights(vb[2, y + 2, pl.ds(8 + z0, CHUNK), :])
            for k in range(5):
                wz[k, y, pl.ds(8 + z0, CHUNK), :] = w[k]
        return carry

    def wz_edge(y, carry):
        for r0 in (0, 8 + CZ):
            w = remesh_weights(vb[2, y + 2, pl.ds(r0, 8), :])
            for k in range(5):
                wz[k, y, pl.ds(r0, 8), :] = w[k]
        return carry

    def wy_one(y, rows):
        for z0, n in rows:
            w = remesh_weights(vb[1, y, pl.ds(8 + z0, n), :])
            for k in range(5):
                wy[k, y, pl.ds(z0, n), :] = w[k]

    def wy_loop(y, carry):
        wy_one(y + 2, ((0, CHUNK), (CHUNK, CHUNK)))
        return carry

    c0 = section_step / 12.0
    cl = section_step * viscosity / 12.0

    def around(buf, c, y, z0, n, dim):
        if dim == 2:
            return [buf[c, y + 2 + k, pl.ds(8 + z0, n), :] for k in (-2, -1, 1, 2)]
        if dim == 1:
            return [buf[c, y + 2, pl.ds(8 + z0 + k, n), :] for k in (-2, -1, 1, 2)]
        f = buf[c, y + 2, pl.ds(8 + z0, n), :]
        lanes = lax.broadcasted_iota(jnp.int32, (n, NX), 1)
        res = []
        for k in (-2, -1, 1, 2):
            r = pltpu.roll(f, (-k) % NX, 1)
            m = lanes >= -k if k < 0 else lanes < NX - k
            res.append(jnp.where(m, r, 0.0))
        return res

    def section_rows(y, rows, dims=(0, 1, 2)):
        for z0, n in rows:
            om = [wb[c, y + 2, pl.ds(8 + z0, n), :] for c in range(3)]
            oms = {d: c0 * om[2 - d] for d in dims}
            for c in range(3):
                acc = om[c] if 0 in dims else sb[c, y, pl.ds(z0, n), :]
                near = None
                far = None
                for dim in dims:
                    a = around(vb, c, y, z0, n, dim)
                    acc = acc + oms[dim] * (8.0 * (a[2] - a[1]) - (a[3] - a[0]))
                    b = around(wb, c, y, z0, n, dim)
                    p = b[1] + b[2]
                    e = b[0] + b[3]
                    near = p if near is None else near + p
                    far = e if far is None else far + e
                acc = acc + cl * (16.0 * near - far - (30.0 * len(dims)) * om[c])
                sb[c, y, pl.ds(z0, n), :] = acc

    RIM = ((0, 8), (CZ - 8, 8))
    half = (CZ - 16) // 2
    MID = ((8, half), (8 + half, half))

    def edge_y(i):
        return jnp.where(i < 2, i, i + CY - 4)

    def run(n, fn):
        def step(i, carry):
            fn(i)
            return carry

        lax.fori_loop(0, n, step, 0)

    lax.fori_loop(0, CY, wx_loop, 0)
    run(CY - 4, lambda i: section_rows(i + 2, MID))
    run(4, lambda i: section_rows(edge_y(i), MID, (0, 1)))

    def p1_wait(s):
        return rcopy(p1r.at[s], p1r.at[s], p1s.at[0], p1v.at[s], (gy, gz))

    def p2_copy(d):
        return rcopy(p2s, p2r.at[d], p2ss.at[d - 1], p2v.at[d], (peer(d), gz))

    @pl.when(in_span)
    def _():
        for s in range(nvb):
            @pl.when(gz != vb0 + s)
            def _():
                p1_wait(s).wait_recv()
        tile = p1r[0]
        for s in range(1, nvb):
            tile = tile + p1r[s]
        p2s[...] = tile
        p2r[0] = tile
        for d in range(1, span):
            p2_copy(d).start()

    for d in range(2):
        @pl.when(up_cond[d][0])
        def _():
            y_copy(0, d, 2).start()
            y_copy(1, d, 2).start()

    lax.fori_loop(0, CY, wz_loop, 0)
    lax.fori_loop(0, CY, wy_loop, 0)

    for d in range(2):
        @pl.when(rt_cond[d][1])
        def _():
            z_copy(d).wait_recv()
            lo = 6 if d == 0 else 8 + CZ

            def unpack(i, carry):
                c = i // 4
                g = i % 4
                for f, buf in ((0, vb), (1, wb)):
                    for j in range(4):
                        buf[c, 2 + 4 * g + j, lo:lo + 2, :] = zr[d, f, c, g, 2 * j:2 * j + 2, :]
                return carry

            lax.fori_loop(0, 12, unpack, 0)

    lax.fori_loop(0, CY, wz_edge, 0)
    run(4, lambda i: section_rows(edge_y(i), RIM, (0, 1)))
    run(CY - 4, lambda i: section_rows(i + 2, RIM))

    for f in range(2):
        for d in range(2):
            @pl.when(up_cond[d][1])
            def _():
                for part in range(2):
                    y_copy(f, d, part).wait_recv()

    run(4, lambda i: section_rows(edge_y(i), RIM, (2,)))
    for y in (0, 1, CY + 2, CY + 3):
        wy_one(y, RIM)

    def p3_copy(d):
        return rcopy(p3s, p3r.at[zc], p3ss.at[d - 1], p3v.at[zc],
                     (lax.rem(zc + d, n_zc) * 8 + plane, gz))

    @pl.when(in_span)
    def _():
        for d in range(1, span):
            rcopy(p2r.at[d], p2r.at[d], p2ss.at[0], p2v.at[d], (gy, gz)).wait_recv()
        tile = p2r[0]
        for d in range(1, span):
            tile = tile + p2r[d]
        p3s[...] = tile
        p3r[zc] = tile

    def smear_rows(ys, spans):
        lhs = []
        for y in ys:
            for c in range(3):
                row = ab[c + 1, pl.ds(y, 1), :]
                for z0, n in spans:
                    lhs.append(tzb[pl.ds(z0, n), :] * row)
        res = dot3(split(jnp.concatenate(lhs, axis=0)), (txb[0], txb[1]), ((1,), (1,)))
        at = 0
        for y in ys:
            for c in range(3):
                for z0, n in spans:
                    sb[c, y, pl.ds(z0, n), :] = sb[c, y, pl.ds(z0, n), :] + res[at:at + n]
                    at += n

    @pl.when(is_src)
    def _():
        tile = p3s[...]
        pv2 = [pick(tile[c:c + 1], tile[4 + c:5 + c]) for c in range(3)]
        src = forces(trig2, chord2, pv2)
        e0 = jnp.zeros((8, 128), F32)
        e1 = e0
        for c in range(3):
            e0 = jnp.where(row8 == c, jnp.broadcast_to(src[c][0:1], (8, 128)), e0)
            e1 = jnp.where(row8 == c, jnp.broadcast_to(src[c][1:2], (8, 128)), e1)
        srcq = jnp.dot(e0, sel[0], precision=HI, preferred_element_type=F32)
        srcq = srcq + jnp.dot(e1, sel[1], precision=HI, preferred_element_type=F32)
        for c in range(3):
            ab[c + 1] = section_step * ab[0] * srcq[c:c + 1, :]
        smear_rows((0, 1, CY - 2, CY - 1), RIM)

    def move_x(y, rows):
        for z0, n in rows:
            for c in range(3):
                f = sb[c, y, pl.ds(z0, n), :]
                g = wx[2, y, pl.ds(z0, n), :] * f
                for k in (0, 1, 3, 4):
                    p = wx[k, y, pl.ds(z0, n), :] * f
                    g = g + pltpu.roll(p, (k - 2) % NX, 1)
                mb[c, y + 2, pl.ds(z0, n), :] = g

    def m_copy(d, part):
        src_y, dst_y = (CY, 0) if d == 0 else (2, CY + 2)
        z0, n = PARTS[part]
        return rcopy(mb.at[:, pl.ds(src_y, 2), pl.ds(z0, n)], mb.at[:, pl.ds(dst_y, 2), pl.ds(z0, n)],
                     ms.at[d, part], mr.at[d, part], (gy + (1 if d == 0 else -1), gz))

    for d in range(2):
        run(2, lambda i: move_x(i + (CY - 2 if d == 0 else 0), RIM))

        @pl.when(up_cond[d][0])
        def _():
            for part in range(2):
                m_copy(d, part).start()

    @pl.when(in_span)
    def _():
        for d in range(1, n_zc):
            p3_copy(d).start()

    @pl.when(is_src)
    def _():
        run((CY - 4) // 4, lambda i: smear_rows([4 * i + 2 + j for j in range(4)], RIM))

    for f in range(2):
        for d in range(2):
            @pl.when(up_cond[d][1])
            def _():
                y_copy(f, d, 2).wait_recv()

    for d in range(2):
        off = CY - 2 if d == 0 else 0
        run(2, lambda i: section_rows(i + off, MID, (2,)))

        @pl.when(is_src)
        def _():
            smear_rows((off, off + 1), MID)

        run(2, lambda i: move_x(i + off, MID))

        @pl.when(up_cond[d][0])
        def _():
            m_copy(d, 2).start()

    run(CY - 4, lambda i: move_x(i + 2, RIM))

    def move_y(y, rows):
        for z0, n in rows:
            w = [wy[k, y + 4 - k, pl.ds(z0, n), :] for k in range(5)]
            for c in range(3):
                g = w[0] * mb[c, y + 4, pl.ds(z0, n), :]
                for k in range(1, 5):
                    g = g + w[k] * mb[c, y + 4 - k, pl.ds(z0, n), :]
                yb[c, y, pl.ds(8 + z0, n), :] = g

    run(CY - 4, lambda i: move_y(i + 2, RIM))
    for d in range(2):
        @pl.when(up_cond[d][1])
        def _():
            for part in range(2):
                m_copy(d, part).wait_recv()

    run(4, lambda i: move_y(edge_y(i), RIM))

    def pack2(i):
        c = i // 4
        g = i % 4
        for j in range(4):
            y = 4 * g + j
            ks[0, c, g, 2 * j:2 * j + 2, :] = yb[c, y, 6 + CZ:8 + CZ, :]
            ks[1, c, g, 2 * j:2 * j + 2, :] = yb[c, y, 8:10, :]

    run(12, pack2)

    def k_copy(d):
        return rcopy(ks.at[d], kr.at[d], kss.at[d], ksr.at[d], (gy, gz + (1 if d == 0 else -1)))

    for d in range(2):
        @pl.when(rt_cond[d][0])
        def _():
            k_copy(d).start()

    @pl.when(is_src)
    def _():
        run((CY - 4) // 2, lambda i: smear_rows((2 * i + 2, 2 * i + 3), MID))

    run(CY - 4, lambda i: move_x(i + 2, MID))
    for y in (0, 1, CY + 2, CY + 3):
        wy_one(y, MID)
    run(CY - 4, lambda i: move_y(i + 2, MID))
    for d in range(2):
        @pl.when(up_cond[d][1])
        def _():
            m_copy(d, 2).wait_recv()

    run(4, lambda i: move_y(edge_y(i), MID))

    def move_z(y, rows):
        for z0, n in rows:
            w = [wz[k, y, pl.ds(8 + z0 + 2 - k, n), :] for k in range(5)]
            for c in range(3):
                g = w[0] * yb[c, y, pl.ds(8 + z0 + 2, n), :]
                for k in range(1, 5):
                    g = g + w[k] * yb[c, y, pl.ds(8 + z0 + 2 - k, n), :]
                out_ref[c, y, pl.ds(z0, n), :] = g

    run(CY, lambda y: move_z(y, MID))

    for s in range(n_zc):
        @pl.when((zc != s) & (s * 8 + plane < NS))
        def _():
            rcopy(p3r.at[s], p3r.at[s], p3ss.at[0], p3v.at[s], (gy, gz)).wait_recv()

    for s in range(n_zc):
        @pl.when(s * 8 + plane < NS)
        def _():
            tall[(s * 8 + plane) // span] = p3r[s]

    for u in range(TURBINES // 2):
        e, o = tall[2 * u], tall[2 * u + 1]
        for c in range(3):
            pvb[c, 3 * u:3 * u + 1, :] = e[c:c + 1]
            pvb[c, 3 * u + 1:3 * u + 2, :] = e[4 + c:5 + c] + o[c:c + 1]
            pvb[c, 3 * u + 2:3 * u + 3, :] = o[4 + c:5 + c]
    n_rows = TURBINES * BLADES * BP // 128
    for r in range(n_rows):
        pvb[3, r:r + 1, :] = chord_ref[128 * r:128 * r + 128].reshape(1, 128)
        pvb[4, r:r + 1, :] = twist_ref[128 * r:128 * r + 128].reshape(1, 128)
    r16 = lax.broadcasted_iota(jnp.int32, (16, 128), 0)
    live = r16 < n_rows
    full = forces(
        trig(r16, jnp.where(live, pvb[4], 0.0)), jnp.where(live, pvb[3], 0.0),
        [jnp.where(live, pvb[c], 0.0) for c in range(3)])
    for r in range(n_rows):
        for c in range(3):
            src_out[c:c + 1, 128 * r:128 * r + 128] = full[c][r:r + 1]

    for d in range(2):
        @pl.when(rt_cond[d][1])
        def _():
            k_copy(d).wait_recv()
            lo = 6 if d == 0 else 8 + CZ

            def unpack2(i):
                c = i // 4
                g = i % 4
                for j in range(4):
                    yb[c, 4 * g + j, lo:lo + 2, :] = kr[d, c, g, 2 * j:2 * j + 2, :]

            run(12, unpack2)

    run(CY, lambda y: move_z(y, RIM))

    for d in range(2):
        @pl.when(rt_cond[d][0])
        def _():
            z_copy(d).wait_send()
            k_copy(d).wait_send()

        @pl.when(up_cond[d][0])
        def _():
            for part in range(3):
                y_copy(0, d, part).wait_send()
                y_copy(1, d, part).wait_send()
                m_copy(d, part).wait_send()

    @pl.when(is_src)
    def _():
        for d in range(1, n_z):
            p1_copy(d).wait_send()

    @pl.when(in_span)
    def _():
        for d in range(1, span):
            p2_copy(d).wait_send()
        for d in range(1, n_zc):
            p3_copy(d).wait_send()


def on_device(n_y, n_z, omega, velocity, owner, cells, frac, chord, twist, angle):
    _, cy, cz, nx = omega.shape
    n_p = owner.shape[0]
    n_zc = n_y // 8
    vm = pl.BlockSpec(memory_space=pltpu.VMEM)
    hb = pl.BlockSpec(memory_space=pl.ANY)
    nvb = max(n_z // 2, 1)
    V = pltpu.VMEM
    D = pltpu.SemaphoreType.DMA
    scratch = [
        V((3, cy + 4, cz + 16, nx), F32),
        V((3, cy + 4, cz + 16, nx), F32),
        V((3, cy, cz, nx), F32),
        V((3, cy + 4, cz, nx), F32),
        V((3, cy, cz + 16, nx), F32),
        V((5, cy, cz, nx), F32),
        V((5, cy + 4, cz, nx), F32),
        V((5, cy, cz + 16, nx), F32),
        V((2, 2, 3, cy // 4, 8, nx), F32),
        V((2, 2, 3, cy // 4, 8, nx), F32),
        V((2, 3, cy // 4, 8, nx), F32),
        V((2, 3, cy // 4, 8, nx), F32),
        V((8, n_p), F32),
        V((2, 128, 128), F32),
        V((8, 128), F32),
        V((nvb, 8, 128), F32),
        V((8, 128), F32),
        V((n_y // TURBINES, 8, 128), F32),
        V((8, 128), F32),
        V((n_zc, 8, 128), F32),
        V((5, 16, 128), F32),
        V((TURBINES, 8, 128), F32),
        V((4, cy, 128), F32),
        V((2, nx, 128), BF),
        V((cz, 128), F32),
        V((n_p,), jnp.int32), V((3, n_p), jnp.int32), V((3, n_p), F32), V((n_p,), F32), V((n_p,), F32),
        pltpu.SMEM((1,), jnp.int32),
        D((12,)), D((2, 2, 3)), D((2, 2, 3)), D((2,)), D((2,)),
        D((n_z - 1,)), D((nvb,)), D((n_y // TURBINES - 1,)), D((n_y // TURBINES,)), D((n_zc - 1,)), D((n_zc,)),
        D((2, 3)), D((2, 3)), D((2,)), D((2,)),
    ]
    out, src = pl.pallas_call(
        functools.partial(kernel, n_y, n_z),
        name="section",
        out_shape=(
            pltpu.VMEM(omega.shape, F32),
            V((3, n_p), F32),
        ),
        in_specs=[hb] * 8,
        out_specs=(vm, vm),
        scratch_shapes=scratch,
        compiler_params=pltpu.CompilerParams(
            collective_id=0, has_side_effects=True, vmem_limit_bytes=60 * 1024 * 1024),
    )(omega, velocity, owner, cells, frac, chord, twist, angle)
    return out, src


def solution(mesh):
    n_y, n_z = mesh.shape["gy"], mesh.shape["gz"]
    field = P(None, "gy", "gz", None)
    return jax.shard_map(
        functools.partial(on_device, n_y, n_z),
        mesh=mesh,
        in_specs=(field, field, P(), P(), P(), P(), P(), P()),
        out_specs=(field, P()),
        check_vma=False,
    )
```
